8 devices in a mesh: rep: 1 (over z), row: 2 (over y), col: 2 (over x), core: 2 (over core).
Axes of the slice: x: 2, y: 2, z: 1, core: 2. Of those that a mesh axis runs over, the one named last changes fastest.
Arguments:
- x: bfloat16 [2, 512, 640], P(None, ('rep', 'row', 'col', 'core'))
- route_idx: int32 [2, 512, 4], P(None, ('rep', 'row', 'col', 'core'))
- gates: float32 [2, 512, 4], P(None, ('rep', 'row', 'col', 'core'))
- w_gate: bfloat16 [128, 640, 640], P(('rep', 'row', 'col', 'core'))
- w_up: bfloat16 [128, 640, 640], P(('rep', 'row', 'col', 'core'))
- w_down: bfloat16 [128, 640, 640], P(('rep', 'row', 'col', 'core'))
- grad_y: bfloat16 [2, 512, 640], P(None, ('rep', 'row', 'col', 'core'))
Outputs:
- output 1: bfloat16 [2, 512, 640], P(None, ('rep', 'row', 'col', 'core'))
- output 2: bfloat16 [2, 512, 640], P(None, ('rep', 'row', 'col', 'core'))
- output 3: float32 [2, 512, 4], P(None, ('rep', 'row', 'col', 'core'))
- output 4: float32 [128, 640, 640], P(('rep', 'row', 'col', 'core'))
- output 5: float32 [128, 640, 640], P(('rep', 'row', 'col', 'core'))
- output 6: float32 [128, 640, 640], P(('rep', 'row', 'col', 'core'))
All inputs are finite; a program needn't handle non-finite values.
Results may differ from the reference program's by a relative error of at most 0.00854886.
Values are sent between devices in bfloat16 or wider.
A program may use at most 1 GiB of HBM per device.

```python
import jax
import jax.numpy as jnp
from jax import lax

D_MODEL = 640
D_FF = 640
EXPERTS = 128
TOP_K = 4
TOK_DEV = 64
N_ROWS = 2
N_COLS = 2
N_CORES = 2

GROUP_SIZE = N_ROWS * N_COLS * N_CORES
TOKENS = GROUP_SIZE * TOK_DEV
CAPACITY = TOK_DEV // 2
CHIP_EXP = EXPERTS // (N_ROWS * N_COLS)
N_HOT = min(CHIP_EXP, TOP_K // 2)
N_COLD = EXPERTS - N_HOT
LOAD_MAX = GROUP_SIZE * CAPACITY


def draw_hot_chips(base_key):
    key_list = jax.random.split(base_key, 4)
    row_first = jax.random.randint(key_list[0], (), 0, N_ROWS)
    col_first = jax.random.randint(key_list[1], (), 0, N_COLS)
    row_second = (row_first + jax.random.randint(key_list[2], (), 1, N_ROWS)) % N_ROWS
    col_second = (col_first + jax.random.randint(key_list[3], (), 1, N_COLS)) % N_COLS
    return row_first * N_COLS + col_first, row_second * N_COLS + col_second


def draw_routing(base_key, hot_chip):
    key_list = jax.random.split(base_key, 4)
    slot_ids = jnp.arange(TOP_K)
    hot_ids = hot_chip * CHIP_EXP + jnp.arange(N_HOT) * (CHIP_EXP // N_HOT)
    sel_keys = jax.random.split(key_list[0], GROUP_SIZE * N_HOT)
    perm_rank = jax.vmap(lambda sub_key: jax.random.permutation(sub_key, TOK_DEV))(sel_keys)
    hot_mask = (perm_rank < CAPACITY).astype(jnp.int32).reshape(GROUP_SIZE, N_HOT, TOK_DEV)
    hot_mask = jnp.transpose(hot_mask, (0, 2, 1))
    hot_count = jnp.sum(hot_mask, axis=2)
    hot_rank = jnp.cumsum(hot_mask, axis=2) - hot_mask
    hot_pick = hot_mask[:, :, :, None] * (hot_rank[:, :, :, None] == slot_ids).astype(jnp.int32)
    hot_route = jnp.sum(hot_pick * hot_ids[None, None, :, None], axis=2)
    is_hot = jnp.zeros((EXPERTS,), jnp.int32).at[hot_ids].set(1)
    cold_sorted = jnp.argsort(is_hot * EXPERTS + jnp.arange(EXPERTS))[:N_COLD]
    cold_keys = jax.random.split(key_list[1], GROUP_SIZE)
    cold_perm = jax.vmap(lambda sub_key: jax.random.permutation(sub_key, cold_sorted))(cold_keys)
    win_start = jax.random.randint(key_list[2], (GROUP_SIZE, 1, 1), 0, N_COLD)
    cold_offset = slot_ids[None, None, :] - hot_count[:, :, None]
    cold_pos = (win_start + jnp.arange(TOK_DEV)[None, :, None] * TOP_K + cold_offset) % N_COLD
    cold_route = jnp.take_along_axis(cold_perm, cold_pos.reshape(GROUP_SIZE, TOK_DEV * TOP_K), axis=1)
    route_ids = jnp.where(cold_offset < 0, hot_route, cold_route.reshape(GROUP_SIZE, TOK_DEV, TOP_K))
    slot_rot = jax.random.randint(key_list[3], (GROUP_SIZE, TOK_DEV, 1), 0, TOP_K)
    route_ids = jnp.take_along_axis(route_ids, (slot_ids - slot_rot) % TOP_K, axis=2)
    return route_ids.reshape(TOKENS, TOP_K).astype(jnp.int32)


def setup_inputs(seed: int = 0, part: int = 0) -> dict:
    base_key = jax.random.fold_in(jax.random.key(seed), part)
    key_list = jax.random.split(base_key, 9)
    hot_first, hot_second = draw_hot_chips(key_list[0])
    route_idx = jnp.stack([draw_routing(key_list[1], hot_first), draw_routing(key_list[2], hot_second)])
    x = jax.random.normal(key_list[3], (2, TOKENS, D_MODEL), jnp.float32).astype(jnp.bfloat16)
    raw_gates = jax.random.uniform(key_list[4], (2, TOKENS, TOP_K), jnp.float32, 1.0, 2.0)
    gates = raw_gates / jnp.sum(raw_gates, axis=2, keepdims=True)
    w_gate = (jax.random.normal(key_list[5], (EXPERTS, D_MODEL, D_FF), jnp.float32) * D_MODEL ** -0.5).astype(jnp.bfloat16)
    w_up = (jax.random.normal(key_list[6], (EXPERTS, D_MODEL, D_FF), jnp.float32) * D_MODEL ** -0.5).astype(jnp.bfloat16)
    w_down = (jax.random.normal(key_list[7], (EXPERTS, D_FF, D_MODEL), jnp.float32) * D_FF ** -0.5).astype(jnp.bfloat16)
    grad_y = jax.random.normal(key_list[8], (2, TOKENS, D_MODEL), jnp.float32).astype(jnp.bfloat16)
    return {"x": x, "route_idx": route_idx, "gates": gates, "w_gate": w_gate, "w_up": w_up, "w_down": w_down, "grad_y": grad_y}


def swiglu_rows(x_rows, d_out, w_gate_e, w_up_e, w_down_e):
    gate_pre = jnp.dot(x_rows, w_gate_e, preferred_element_type=jnp.float32).astype(jnp.bfloat16)
    up_pre = jnp.dot(x_rows, w_up_e, preferred_element_type=jnp.float32).astype(jnp.bfloat16)
    gate_f = gate_pre.astype(jnp.float32)
    up_f = up_pre.astype(jnp.float32)
    sigmoid_g = jax.nn.sigmoid(gate_f)
    hidden = (gate_f * sigmoid_g * up_f).astype(jnp.bfloat16)
    exp_out = jnp.dot(hidden, w_down_e, preferred_element_type=jnp.float32).astype(jnp.bfloat16)
    d_act = jnp.dot(d_out, w_down_e.T, preferred_element_type=jnp.float32)
    d_up = (d_act * gate_f * sigmoid_g).astype(jnp.bfloat16)
    d_gate = (d_act * up_f * sigmoid_g * (1.0 + gate_f * (1.0 - sigmoid_g))).astype(jnp.bfloat16)
    d_in = (jnp.dot(d_gate, w_gate_e.T, preferred_element_type=jnp.float32) + jnp.dot(d_up, w_up_e.T, preferred_element_type=jnp.float32)).astype(jnp.bfloat16)
    g_gate = jnp.dot(x_rows.T, d_gate, preferred_element_type=jnp.float32)
    g_up = jnp.dot(x_rows.T, d_up, preferred_element_type=jnp.float32)
    g_down = jnp.dot(hidden.T, d_out, preferred_element_type=jnp.float32)
    return exp_out, d_in, g_gate, g_up, g_down


def microbatch(x, route_ids, gates, grad_y, w_gate, w_up, w_down):
    token_ids = jnp.arange(TOKENS)
    member = jnp.zeros((TOKENS, EXPERTS), jnp.int32).at[token_ids[:, None], route_ids].set(1)
    slot_rank = jnp.cumsum(member, axis=0) - member
    slot_pos = jnp.take_along_axis(slot_rank, route_ids, axis=1)
    slot_owner = jnp.full((EXPERTS * LOAD_MAX,), TOKENS * TOP_K, jnp.int32)
    slot_owner = slot_owner.at[(route_ids * LOAD_MAX + slot_pos).reshape(-1)].set(jnp.arange(TOKENS * TOP_K))
    slot_owner = slot_owner.reshape(EXPERTS, LOAD_MAX)
    x_pad = jnp.concatenate([x, jnp.zeros((1, D_MODEL), x.dtype)])
    dy_pad = jnp.concatenate([grad_y, jnp.zeros((1, D_MODEL), grad_y.dtype)])
    gate_pad = jnp.concatenate([gates.reshape(-1), jnp.zeros((1,), jnp.float32)])

    def one_expert(accums, per_expert):
        y_acc, dx_acc, dg_acc = accums
        slot_ids, w_gate_e, w_up_e, w_down_e = per_expert
        tok_rows = slot_ids // TOP_K
        row_gate = gate_pad[slot_ids]
        x_rows = x_pad[tok_rows]
        dy_rows = dy_pad[tok_rows].astype(jnp.float32)
        d_out = (row_gate[:, None] * dy_rows).astype(jnp.bfloat16)
        exp_out, d_in, g_gate, g_up, g_down = swiglu_rows(x_rows, d_out, w_gate_e, w_up_e, w_down_e)
        out_f = exp_out.astype(jnp.float32)
        y_acc = y_acc.at[tok_rows].add(row_gate[:, None] * out_f)
        dx_acc = dx_acc.at[tok_rows].add(d_in.astype(jnp.float32))
        dg_acc = dg_acc.at[slot_ids].add(jnp.sum(dy_rows * out_f, axis=1))
        return (y_acc, dx_acc, dg_acc), (g_gate, g_up, g_down)

    init_acc = (jnp.zeros((TOKENS + 1, D_MODEL), jnp.float32), jnp.zeros((TOKENS + 1, D_MODEL), jnp.float32), jnp.zeros((TOKENS * TOP_K + 1,), jnp.float32))
    final_acc, grads = lax.scan(one_expert, init_acc, (slot_owner, w_gate, w_up, w_down))
    y_acc, dx_acc, dg_acc = final_acc
    y_out = y_acc[:TOKENS].astype(jnp.bfloat16)
    dx_out = dx_acc[:TOKENS].astype(jnp.bfloat16)
    dg_out = dg_acc[:TOKENS * TOP_K].reshape(TOKENS, TOP_K)
    return y_out, dx_out, dg_out, grads[0], grads[1], grads[2]


def reference(x, route_idx, gates, w_gate, w_up, w_down, grad_y):
    mb_first = microbatch(x[0], route_idx[0], gates[0], grad_y[0], w_gate, w_up, w_down)
    mb_second = microbatch(x[1], route_idx[1], gates[1], grad_y[1], w_gate, w_up, w_down)
    return (jnp.stack([mb_first[0], mb_second[0]]), jnp.stack([mb_first[1], mb_second[1]]), jnp.stack([mb_first[2], mb_second[2]]), mb_first[3] + mb_second[3], mb_first[4] + mb_second[4], mb_first[5] + mb_second[5])
```

```python
import functools

import jax
import jax.numpy as jnp
from jax import lax
from jax.experimental import pallas as pl
from jax.experimental.pallas import tpu as pltpu
from jax.sharding import PartitionSpec as P

GROUP_AXES = ("row", "col", "core")
ALL_AXES = ("rep", "row", "col", "core")
MESH = pl.DeviceIdType.MESH
F32, BF16, I32 = jnp.float32, jnp.bfloat16, jnp.int32

N_DEV = 8
BLK = 128
TOK = N_DEV * BLK
TOP_K = 4
LOC = 16
DIM = 640
GATHER = 128
COMB = 256
SMALL, BIG = 64, 256
ROWS = 4864
SLAB = 640
RING = 4
VMEM_MAX = 67043328


def dot(a, b, dims=((1,), (0,))):
    return lax.dot_general(a, b, (dims, ((), ())), preferred_element_type=F32)


def gather_kernel(x_ref, gy_ref, meta_ref, xgy_ref, mall_ref, local_sem, send_sem, recv_sem):
    row, col, core = (lax.axis_index(a) for a in GROUP_AXES)
    sib = {"row": row, "col": col, "core": 1 - core}
    xn = {"row": row, "col": 1 - col, "core": core}
    yn = {"row": 1 - row, "col": col, "core": core}

    def index(r, c):
        return (r * 2 + c) * 2 + core

    blocks = {"own": index(row, col), "xn": index(row, 1 - col), "yn": index(1 - row, col), "diag": index(1 - row, 1 - col)}
    pair = {k: b + 1 - 2 * core for k, b in blocks.items()}
    pieces = ("x", "gy", "meta")

    def place(piece, blk):
        if piece == "meta":
            return mall_ref.at[blk]
        return xgy_ref.at[blk, :, pl.ds(0 if piece == "x" else DIM, DIM)]

    own_src = {"x": x_ref, "gy": gy_ref, "meta": meta_ref}

    barrier = pltpu.get_barrier_semaphore()
    for peer in (sib, xn, yn):
        pl.semaphore_signal(barrier, inc=1, device_id=peer, device_id_type=MESH)
    pl.semaphore_wait(barrier, 3)

    local = []
    for i, p in enumerate(pieces):
        local.append(pltpu.make_async_copy(own_src[p], place(p, blocks["own"]), local_sem.at[i]))
        local[-1].start()

    names = [("x", "own", p) for p in pieces] + [("y", "own", p) for p in pieces]
    names += [("x", "yn", "gy"), ("y", "xn", "x"), ("y", "xn", "meta")]
    names += [("s", b, p) for b in ("own", "xn", "yn", "diag") for p in pieces]
    number = {n: i for i, n in enumerate(names)}
    peer_of = {"x": xn, "y": yn, "s": sib}

    def copy(name):
        link, b, p = name
        i = number[name]
        src = own_src[p] if b == "own" else place(p, blocks[b])
        return pltpu.make_async_remote_copy(
            src_ref=src, dst_ref=place(p, blocks[b]), send_sem=send_sem.at[i], recv_sem=recv_sem.at[i],
            device_id=peer_of[link], device_id_type=MESH)

    copies = {n: copy(n) for n in names}
    for n in (("x", "own", "meta"), ("y", "own", "meta"), ("x", "own", "x"), ("y", "own", "gy"), ("x", "own", "gy"), ("y", "own", "x"),
              ("s", "own", "meta"), ("s", "own", "x"), ("s", "own", "gy")):
        copies[n].start()

    def arrived(link, b, p):
        copies[(link, b, p)].wait_recv()

    arrived("x", "own", "meta")
    copies[("y", "xn", "meta")].start()
    copies[("s", "xn", "meta")].start()
    arrived("y", "own", "meta")
    copies[("s", "yn", "meta")].start()
    arrived("x", "own", "x")
    copies[("y", "xn", "x")].start()
    copies[("s", "xn", "x")].start()
    arrived("y", "own", "gy")
    copies[("x", "yn", "gy")].start()
    copies[("s", "yn", "gy")].start()
    arrived("x", "own", "gy")
    copies[("s", "xn", "gy")].start()
    arrived("y", "own", "x")
    copies[("s", "yn", "x")].start()
    arrived("y", "xn", "meta")
    copies[("s", "diag", "meta")].start()
    arrived("y", "xn", "x")
    copies[("s", "diag", "x")].start()
    arrived("x", "yn", "gy")
    copies[("s", "diag", "gy")].start()
    for b in ("own", "xn", "yn", "diag"):
        for p in pieces:
            arrived("s", b, p)
    for n in names:
        copies[n].wait_send()
    for c in local:
        c.wait()


def all_gather_tokens(x_loc, gy_loc, meta):
    n_copies = 21
    vmem = pl.BlockSpec(memory_space=pltpu.VMEM)
    return pl.pallas_call(
        gather_kernel,
        out_shape=(jax.ShapeDtypeStruct((N_DEV, BLK, 2 * DIM), BF16), jax.ShapeDtypeStruct((N_DEV, 8, BLK), F32)),
        in_specs=[vmem] * 3,
        out_specs=(vmem, vmem),
        scratch_shapes=[pltpu.SemaphoreType.DMA((3,)), pltpu.SemaphoreType.DMA((n_copies,)), pltpu.SemaphoreType.DMA((n_copies,))],
        compiler_params=pltpu.CompilerParams(collective_id=0, has_side_effects=True),
        name="token_gather",
    )(x_loc, gy_loc, meta)


def expert_kernel(meta_ref, xgy_ref, wg_hbm, wu_hbm, wd_hbm, sy_ref, sdx_ref, rows_hbm, cnt_ref,
                  wgu, wd, xs, gys, gcol, os_, ps, dgcol, pos, pos_t, gate_row, off_s, stage_s, stage_b, w_sem, s_sem, b_sem):
    row, col, core = (lax.axis_index(a) for a in GROUP_AXES)
    first = ((row * 2 + col) * 2 + core) * LOC

    def weights(e):
        slot = lax.rem(e, RING)
        return (pltpu.make_async_copy(wg_hbm.at[e], wgu.at[slot, :, pl.ds(0, DIM)], w_sem.at[slot, 0]),
                pltpu.make_async_copy(wu_hbm.at[e], wgu.at[slot, :, pl.ds(DIM, DIM)], w_sem.at[slot, 1]),
                pltpu.make_async_copy(wd_hbm.at[e], wd.at[slot], w_sem.at[slot, 2]))

    for e in range(RING):
        for c in weights(jnp.int32(e)):
            c.start()

    local = [jnp.concatenate([meta_ref[n, j:j + 1, :] for n in range(N_DEV)], axis=1) - first.astype(F32) for j in range(TOP_K)]
    for j in range(TOP_K):
        gate_row[j:j + 1, :] = jnp.concatenate([meta_ref[n, TOP_K + j:TOP_K + j + 1, :] for n in range(N_DEV)], axis=1)
    eid = lax.broadcasted_iota(I32, (LOC, TOK), 0).astype(F32)
    member = jnp.zeros((LOC, TOK), F32)
    for j in range(TOP_K):
        member = member + jnp.where(local[j] == eid, 1.0, 0.0)
    upper = (lax.broadcasted_iota(I32, (BLK, BLK), 0) < lax.broadcasted_iota(I32, (BLK, BLK), 1))
    upper = jnp.where(upper, 1.0, 0.0).astype(BF16)
    parts = [member[:, b * BLK:(b + 1) * BLK] for b in range(N_DEV)]
    before = dot(jnp.concatenate(parts, axis=0).astype(BF16), upper)
    run = jnp.zeros((LOC, 1), F32)
    ranks = []
    for b in range(N_DEV):
        ranks.append(before[b * LOC:(b + 1) * LOC, :] + run)
        run = run + jnp.sum(parts[b], axis=1, keepdims=True)
    rank = jnp.concatenate(ranks, axis=1)
    erow = lax.broadcasted_iota(I32, (LOC, 1), 0)
    off_v = jnp.zeros((LOC, 1), F32)
    off = jnp.int32(0)
    for e in range(LOC):
        cnt = jnp.sum(jnp.where(erow == e, run, 0.0)).astype(I32)
        cnt_ref[e] = cnt
        off_s[e] = off
        off_v = jnp.where(erow == e, off.astype(F32), off_v)
        off = off + ((cnt + 15) // 16) * 16
    n_comb = (off + COMB - 1) // COMB
    place = rank + off_v
    for j in range(TOP_K):
        mine = jnp.full((1, TOK), -1.0, F32)
        for e in range(LOC):
            mine = jnp.where(local[j] == float(e), place[e:e + 1, :], mine)
        pos[j:j + 1, :] = mine
    for b in range(N_DEV):
        blk = jnp.concatenate([pos[:, b * BLK:(b + 1) * BLK], jnp.zeros((BLK - 8, BLK), F32)], axis=0)
        pos_t[b * BLK:(b + 1) * BLK, :] = blk.T

    sy_ref[...] = jnp.zeros_like(sy_ref)
    sdx_ref[...] = jnp.zeros_like(sdx_ref)

    def gather(i, carry):
        r0 = pl.multiple_of(i * GATHER, GATHER)
        rid = (r0 + lax.broadcasted_iota(I32, (GATHER, 1), 0)).astype(F32)
        picks, gsum = [], jnp.zeros((GATHER, 256), F32)
        for kb in range(TOK // 256):
            lanes = slice(kb * 256, (kb + 1) * 256)
            hit, gsel = None, gsum
            for j in range(TOP_K):
                m = pos[j:j + 1, lanes] == rid
                hit = m if hit is None else hit | m
                gsel = jnp.where(m, gate_row[j:j + 1, lanes], gsel)
            gsum = gsel
            picks.append(jnp.where(hit, 1.0, 0.0).astype(BF16))
        got = dot(jnp.concatenate(picks, axis=1), xgy_ref[...].reshape(TOK, 2 * DIM)).astype(BF16)
        here = pl.ds(r0, GATHER)
        xs[here, :] = got[:, :DIM]
        gys[here, :] = got[:, DIM:]
        gcol[here, :] = jnp.sum(gsum, axis=1, keepdims=True)
        os_[here, :] = jnp.zeros((GATHER, DIM), BF16)
        ps[here, :] = jnp.zeros((GATHER, DIM), BF16)
        dgcol[here, :] = jnp.zeros((GATHER, 1), F32)
        return carry

    lax.fori_loop(0, 2 * n_comb, gather, 0)

    def chunk(size, base, slot, stage):
        here = pl.ds(pl.multiple_of(base, 16), size)
        x = xs[here, :]
        gy = gys[here, :].astype(F32)
        q = (gcol[here, :] * gy).astype(BF16)
        uv = dot(x, wgu[slot])
        u = uv[:, :DIM].astype(BF16).astype(F32)
        v = uv[:, DIM:].astype(BF16).astype(F32)
        s = jax.nn.sigmoid(u)
        a = (u * s * v).astype(BF16)
        o = dot(a, wd[slot]).astype(BF16)
        r = dot(q, wd[slot], ((1,), (1,)))
        dv = (r * u * s).astype(BF16)
        du = (r * v * s * (1.0 + u * (1.0 - s))).astype(BF16)
        duv = jnp.concatenate([du, dv], axis=1)
        p = dot(duv, wgu[slot], ((1,), (1,))).astype(BF16)
        os_[here, :] = o
        ps[here, :] = p
        dgcol[here, :] = jnp.sum(gy * o.astype(F32), axis=1, keepdims=True)
        stage[:, 0:DIM] = x
        stage[:, DIM:2 * DIM] = a
        stage[:, 2 * DIM:3 * DIM] = q
        stage[:, 3 * DIM:5 * DIM] = duv

    def small_out(e, row0):
        return pltpu.make_async_copy(stage_s.at[lax.rem(e, 2)], rows_hbm.at[e, pl.ds(pl.multiple_of(row0, 64), SMALL)], s_sem.at[lax.rem(e, 2)])

    def expert(e, carry):
        slot = lax.rem(e, RING)
        cnt, base = cnt_ref[e], off_s[e]
        for c in weights(e):
            c.wait()
        n_big = (cnt + BIG - SMALL - 1) // BIG

        def big(b, c2):
            chunk(BIG, base + b * BIG, slot, stage_b)
            out = pltpu.make_async_copy(stage_b, rows_hbm.at[e, pl.ds(pl.multiple_of(b * BIG, BIG), BIG)], b_sem)
            out.start()
            out.wait()
            return c2

        lax.fori_loop(0, n_big, big, 0)

        @pl.when(e >= 2)
        def _():
            small_out(e, 0).wait()

        chunk(SMALL, base + n_big * BIG, slot, stage_s.at[lax.rem(e, 2)])
        small_out(e, n_big * BIG).start()

        @pl.when(e + RING < LOC)
        def _():
            for c in weights(e + RING):
                c.start()

        return carry

    lax.fori_loop(0, LOC, expert, 0)
    small_out(0, 0).wait()
    small_out(1, 0).wait()

    def combine(i, carry):
        r0 = pl.multiple_of(i * COMB, COMB)
        here = pl.ds(r0, COMB)
        go = gcol[here, :] * os_[here, :].astype(F32)
        hi = go.astype(BF16)
        rem = go - hi.astype(F32)
        mid = rem.astype(BF16)
        low = (rem - mid.astype(F32)).astype(BF16)
        triple = jnp.concatenate([hi, mid, low], axis=0)
        p = ps[here, :]
        dg = dgcol[here, :]
        rid_l = (r0 + lax.broadcasted_iota(I32, (1, COMB), 1)).astype(F32)
        rid_s = (r0 + lax.broadcasted_iota(I32, (COMB, 1), 0)).astype(F32)
        for r in range(2):
            for c in range(2):
                for k in range(2):
                    n = (r * 2 + c) * 2 + k
                    toks = slice(n * BLK, (n + 1) * BLK)
                    hit = None
                    for j in range(TOP_K):
                        m = pos_t[toks, j:j + 1] == rid_l
                        hit = m if hit is None else hit | m
                    pick = jnp.where(hit, 1.0, 0.0).astype(BF16)
                    far = lax.rem(core + k, 2)
                    rel = lax.rem(row + r, 2) * 2 + lax.rem(col + c, 2)
                    sy_ref[far, rel, 0:BLK, :] += dot(jnp.concatenate([pick] * 3, axis=1), triple)
                    sdx_ref[far, rel, :, :] += dot(pick, p)
                    for j in range(TOP_K):
                        m = pos[j:j + 1, toks] == rid_s
                        sy_ref[far, rel, BLK + j:BLK + j + 1, 0:BLK] += jnp.sum(jnp.where(m, dg, 0.0), axis=0, keepdims=True)
        return carry

    lax.fori_loop(0, n_comb, combine, 0)


def run_experts(meta_all, xgy, w_gate, w_up, w_down):
    vmem = pl.BlockSpec(memory_space=pltpu.VMEM)
    hbm = pl.BlockSpec(memory_space=pl.ANY)
    return pl.pallas_call(
        expert_kernel,
        out_shape=(jax.ShapeDtypeStruct((2, 4, BLK + 8, DIM), F32), jax.ShapeDtypeStruct((2, 4, BLK, DIM), F32),
                   jax.ShapeDtypeStruct((LOC, SLAB, 5 * DIM), BF16), jax.ShapeDtypeStruct((LOC,), I32)),
        in_specs=[vmem, vmem, hbm, hbm, hbm],
        out_specs=(vmem, vmem, hbm, pl.BlockSpec(memory_space=pltpu.SMEM)),
        scratch_shapes=[
            pltpu.VMEM((RING, DIM, 2 * DIM), BF16), pltpu.VMEM((RING, DIM, DIM), BF16),
            pltpu.VMEM((ROWS, DIM), BF16), pltpu.VMEM((ROWS, DIM), BF16), pltpu.VMEM((ROWS, 1), F32),
            pltpu.VMEM((ROWS, DIM), BF16), pltpu.VMEM((ROWS, DIM), BF16), pltpu.VMEM((ROWS, 1), F32),
            pltpu.VMEM((8, TOK), F32), pltpu.VMEM((TOK, BLK), F32), pltpu.VMEM((8, TOK), F32),
            pltpu.SMEM((LOC,), I32),
            pltpu.VMEM((2, SMALL, 5 * DIM), BF16), pltpu.VMEM((BIG, 5 * DIM), BF16),
            pltpu.SemaphoreType.DMA((RING, 3)), pltpu.SemaphoreType.DMA((2,)), pltpu.SemaphoreType.DMA,
        ],
        compiler_params=pltpu.CompilerParams(vmem_limit_bytes=VMEM_MAX),
        cost_estimate=pl.CostEstimate(flops=6_000_000_000, bytes_accessed=60_000_000, transcendentals=0),
        name="expert_rows",
    )(meta_all, xgy, w_gate, w_up, w_down)


def wgrad_kernel(lo, hi, n_alias, cnt_ref, rows_hbm, *refs):
    gg_hbm, gu_hbm, gd_hbm = refs[n_alias:n_alias + 3]
    small, big, out_gu, out_d, r_sem, b_sem, o_sem = refs[n_alias + 3:]

    def rows_in(i):
        return pltpu.make_async_copy(rows_hbm.at[lo + i, pl.ds(0, SMALL)], small.at[lax.rem(i, 2)], r_sem.at[lax.rem(i, 2)])

    def results(i):
        slot, e = lax.rem(i, 2), lo + i
        return (pltpu.make_async_copy(out_gu.at[slot, :, pl.ds(0, DIM)], gg_hbm.at[e], o_sem.at[slot, 0]),
                pltpu.make_async_copy(out_gu.at[slot, :, pl.ds(DIM, DIM)], gu_hbm.at[e], o_sem.at[slot, 1]),
                pltpu.make_async_copy(out_d.at[slot], gd_hbm.at[e], o_sem.at[slot, 2]))

    def products(ref, size, left):
        keep = lax.broadcasted_iota(I32, (size, 1), 0) < left
        part = lambda a, b: jnp.where(keep, ref[:, a * DIM:b * DIM], 0.0).astype(BF16)
        x, a, q, duv = part(0, 1), part(1, 2), part(2, 3), part(3, 5)
        return dot(x, duv, ((0,), (0,))), dot(a, q, ((0,), (0,)))

    rows_in(0).start()

    def expert(i, carry):
        slot = lax.rem(i, 2)
        cnt = cnt_ref[lo + i]
        rows_in(i).wait()

        @pl.when(i + 1 < hi - lo)
        def _():
            rows_in(i + 1).start()

        @pl.when(i >= 2)
        def _():
            for c in results(i - 2):
                c.wait()

        @pl.when(cnt <= SMALL)
        def _():
            g1, g2 = products(small.at[slot], SMALL, cnt)
            out_gu[slot] = g1
            out_d[slot] = g2

        @pl.when(cnt > SMALL)
        def _():
            def piece(b, c2):
                cp = pltpu.make_async_copy(rows_hbm.at[lo + i, pl.ds(pl.multiple_of(b * BIG, BIG), BIG)], big, b_sem)
                cp.start()
                cp.wait()
                g1, g2 = products(big, BIG, cnt - b * BIG)

                @pl.when(b == 0)
                def _():
                    out_gu[slot] = g1
                    out_d[slot] = g2

                @pl.when(b > 0)
                def _():
                    out_gu[slot] += g1
                    out_d[slot] += g2

                return c2

            lax.fori_loop(0, (cnt + BIG - 1) // BIG, piece, 0)

        for c in results(i):
            c.start()
        return carry

    lax.fori_loop(0, hi - lo, expert, 0)
    for i in (hi - lo - 2, hi - lo - 1):
        for c in results(jnp.int32(i)):
            c.wait()


def weight_grads(lo, hi, cnt, rows, earlier=()):
    hbm = pl.BlockSpec(memory_space=pl.ANY)
    out = jax.ShapeDtypeStruct((LOC, DIM, DIM), F32)
    return pl.pallas_call(
        functools.partial(wgrad_kernel, lo, hi, len(earlier)),
        out_shape=(out, out, out),
        in_specs=[pl.BlockSpec(memory_space=pltpu.SMEM), hbm] + [hbm] * len(earlier),
        out_specs=(hbm, hbm, hbm),
        input_output_aliases={2 + i: i for i in range(len(earlier))},
        scratch_shapes=[
            pltpu.VMEM((2, SMALL, 5 * DIM), BF16), pltpu.VMEM((BIG, 5 * DIM), BF16),
            pltpu.VMEM((2, DIM, 2 * DIM), F32), pltpu.VMEM((2, DIM, DIM), F32),
            pltpu.SemaphoreType.DMA((2,)), pltpu.SemaphoreType.DMA, pltpu.SemaphoreType.DMA((2, 3)),
        ],
        compiler_params=pltpu.CompilerParams(vmem_limit_bytes=30 * 1024 * 1024),
        cost_estimate=pl.CostEstimate(flops=(hi - lo) * 400_000_000, bytes_accessed=(hi - lo) * 5_000_000, transcendentals=0),
        name="weight_grads",
    )(cnt, rows, *earlier)


def solution(mesh):
    tok_spec = P(None, ALL_AXES, None)
    w_spec = P(ALL_AXES, None, None)

    def swap(value, axis):
        return lax.ppermute(value, axis, [(0, 1), (1, 0)])

    def moe_layer(x, route_idx, gates, w_gate, w_up, w_down, grad_y):
        tok_dev = x.shape[1]
        flat = lambda a: a.reshape(2 * tok_dev, -1)
        meta = jnp.concatenate([flat(route_idx).astype(F32).T, flat(gates).T], axis=0)
        xgy, meta_all = all_gather_tokens(flat(x), flat(grad_y), meta)
        sum_y, sum_dx, rows, cnt = run_experts(meta_all, xgy, w_gate, w_up, w_down)
        chip_y = sum_y[0] + swap(sum_y[1], "core")
        chip_dx = sum_dx[0] + swap(sum_dx[1], "core")
        y_in = swap(chip_y[1::2], "col")
        dx_in = swap(chip_dx[2:], "row")
        early = weight_grads(0, 10, cnt, rows)
        y_far = swap(chip_y[2] + y_in[1], "row")
        dx_far = swap(chip_dx[1] + dx_in[1], "col")
        g_gate, g_up, g_down = weight_grads(10, LOC, cnt, rows, early)
        y_sum = chip_y[0] + y_in[0] + y_far
        dx_sum = chip_dx[0] + dx_in[0] + dx_far
        y = y_sum[:BLK].astype(BF16).reshape(x.shape)
        dx = dx_sum.astype(BF16).reshape(x.shape)
        dg = y_sum[BLK:BLK + TOP_K, :BLK].T.reshape(gates.shape)
        return y, dx, dg, g_gate, g_up, g_down

    return jax.shard_map(moe_layer, mesh=mesh, in_specs=(tok_spec, tok_spec, tok_spec, w_spec, w_spec, w_spec, tok_spec), out_specs=(tok_spec, tok_spec, tok_spec, w_spec, w_spec, w_spec), check_vma=False)
```

```python
import functools

import jax
import jax.numpy as jnp
from jax import lax
from jax.experimental import pallas as pl
from jax.experimental.pallas import tpu as pltpu
from jax.sharding import PartitionSpec as P

GROUP_AXES = ("row", "col", "core")
ALL_AXES = ("rep", "row", "col", "core")
MESH = pl.DeviceIdType.MESH
F32, BF16, I32 = jnp.float32, jnp.bfloat16, jnp.int32

N_DEV = 8
BLK = 128
TOK = N_DEV * BLK
TOP_K = 4
LOC = 16
DIM = 640
GATHER = 128
COMB = 256
SMALL, BIG = 32, 256
ROWS = 4864
SLAB = 640
RING = 4
PIECE = 288
VMEM_MAX = 67043328


def dot(a, b, dims=((1,), (0,))):
    return lax.dot_general(a, b, (dims, ((), ())), preferred_element_type=F32)


def gather_kernel(x_hbm, gy_hbm, route_ref, gate_ref, xg_hbm, mall_ref, land, own_meta, in_sem, out_sem, meta_sem, send_sem, recv_sem):
    row, col, core = (lax.axis_index(a) for a in GROUP_AXES)
    sib = {"row": row, "col": col, "core": 1 - core}
    xn = {"row": row, "col": 1 - col, "core": core}
    yn = {"row": 1 - row, "col": col, "core": core}

    def index(r, c):
        return (r * 2 + c) * 2 + core

    blocks = {"own": index(row, col), "xn": index(row, 1 - col), "yn": index(1 - row, col), "diag": index(1 - row, 1 - col)}
    pair = {k: b + 1 - 2 * core for k, b in blocks.items()}
    pieces = ("x", "gy", "meta")

    def place(piece, blk):
        if piece == "meta":
            return mall_ref.at[blk]
        return land.at[0 if piece == "x" else 1, blk]

    loads = [pltpu.make_async_copy(x_hbm, place("x", blocks["own"]), in_sem.at[0]),
             pltpu.make_async_copy(gy_hbm, place("gy", blocks["own"]), in_sem.at[1])]
    for c in loads:
        c.start()
    own_meta[0:TOP_K, :] = jnp.concatenate([route_ref[0], route_ref[1]], axis=1).astype(F32)
    own_meta[TOP_K:2 * TOP_K, :] = jnp.concatenate([gate_ref[0], gate_ref[1]], axis=1)

    barrier = pltpu.get_barrier_semaphore()
    for peer in (sib, xn, yn):
        pl.semaphore_signal(barrier, inc=1, device_id=peer, device_id_type=MESH)
    pl.semaphore_wait(barrier, 3)

    meta_copy = pltpu.make_async_copy(own_meta, place("meta", blocks["own"]), meta_sem)
    meta_copy.start()

    names = [("x", "own", p) for p in pieces] + [("y", "own", p) for p in pieces]
    names += [("x", "yn", "gy"), ("y", "xn", "x"), ("y", "xn", "meta")]
    names += [("s", b, p) for b in ("own", "xn", "yn", "diag") for p in pieces]
    number = {n: i for i, n in enumerate(names)}
    peer_of = {"x": xn, "y": yn, "s": sib}

    def copy(name):
        link, b, p = name
        i = number[name]
        src = own_meta if b == "own" and p == "meta" else place(p, blocks[b])
        return pltpu.make_async_remote_copy(
            src_ref=src, dst_ref=place(p, blocks[b]), send_sem=send_sem.at[i], recv_sem=recv_sem.at[i],
            device_id=peer_of[link], device_id_type=MESH)

    copies = {n: copy(n) for n in names}
    stores = []

    def store(p, blk):
        half = 0 if p == "x" else 1
        stores.append(pltpu.make_async_copy(land.at[half, blk], xg_hbm.at[half, blk], out_sem.at[len(stores)]))
        stores[-1].start()

    copies[("x", "own", "meta")].start()
    copies[("y", "own", "meta")].start()
    copies[("s", "own", "meta")].start()
    loads[0].wait()
    copies[("x", "own", "x")].start()
    loads[1].wait()
    for n in (("y", "own", "gy"), ("x", "own", "gy"), ("y", "own", "x"), ("s", "own", "x"), ("s", "own", "gy")):
        copies[n].start()
    store("x", blocks["own"])
    store("gy", blocks["own"])

    def arrived(link, b, p, onward, blk):
        copies[(link, b, p)].wait_recv()
        for n in onward:
            copies[n].start()
        if p != "meta":
            store(p, blk)

    arrived("x", "own", "meta", [("y", "xn", "meta"), ("s", "xn", "meta")], None)
    arrived("y", "own", "meta", [("s", "yn", "meta")], None)
    arrived("x", "own", "x", [("y", "xn", "x"), ("s", "xn", "x")], blocks["xn"])
    arrived("y", "own", "gy", [("x", "yn", "gy"), ("s", "yn", "gy")], blocks["yn"])
    arrived("s", "own", "x", [], pair["own"])
    arrived("s", "own", "gy", [], pair["own"])
    arrived("s", "xn", "x", [], pair["xn"])
    arrived("s", "yn", "gy", [], pair["yn"])
    arrived("x", "own", "gy", [("s", "xn", "gy")], blocks["xn"])
    arrived("y", "own", "x", [("s", "yn", "x")], blocks["yn"])
    arrived("y", "xn", "meta", [("s", "diag", "meta")], None)
    arrived("s", "xn", "gy", [], pair["xn"])
    arrived("s", "yn", "x", [], pair["yn"])
    arrived("y", "xn", "x", [("s", "diag", "x")], blocks["diag"])
    arrived("x", "yn", "gy", [("s", "diag", "gy")], blocks["diag"])
    for b in ("own", "xn", "yn", "diag"):
        arrived("s", b, "meta", [], None)
    arrived("s", "diag", "x", [], pair["diag"])
    arrived("s", "diag", "gy", [], pair["diag"])
    for n in names:
        copies[n].wait_send()
    meta_copy.wait()
    for c in stores:
        c.wait()


def all_gather_tokens(x_loc, gy_loc, route, gates):
    n_copies = 21
    vmem = pl.BlockSpec(memory_space=pltpu.VMEM)
    hbm = pl.BlockSpec(memory_space=pl.ANY)
    return pl.pallas_call(
        gather_kernel,
        out_shape=(jax.ShapeDtypeStruct((2, N_DEV, BLK, DIM), BF16), jax.ShapeDtypeStruct((N_DEV, 8, BLK), F32)),
        in_specs=[hbm, hbm, vmem, vmem],
        out_specs=(hbm, vmem),
        scratch_shapes=[pltpu.VMEM((2, N_DEV, BLK, DIM), BF16), pltpu.VMEM((8, BLK), F32), pltpu.SemaphoreType.DMA((2,)),
                        pltpu.SemaphoreType.DMA((16,)), pltpu.SemaphoreType.DMA,
                        pltpu.SemaphoreType.DMA((n_copies,)), pltpu.SemaphoreType.DMA((n_copies,))],
        compiler_params=pltpu.CompilerParams(collective_id=0, has_side_effects=True),
        name="token_gather",
    )(x_loc, gy_loc, route, gates)


def three_parts(value):
    hi = value.astype(BF16).astype(F32)
    mid = (value - hi).astype(BF16).astype(F32)
    return hi, mid, value - hi - mid


def expert_kernel(meta_ref, xg_hbm, wg_hbm, wu_hbm, wd_hbm, keep_y, send_y, keep_dx, send_dx, rows_hbm, cnt_ref,
                  xgy, mt, wgu, wd, xs, gys, mrow, os_, ps, gcol, pos, pos_t, tri, sy, sdx, dacc, off_s, stage_s, stage_b,
                  x_sem, w_sem, s_sem, b_sem, out_sem):
    row, col, core = (lax.axis_index(a) for a in GROUP_AXES)
    first = ((row * 2 + col) * 2 + core) * LOC

    def weights(e):
        slot = lax.rem(e, RING)
        return (pltpu.make_async_copy(wg_hbm.at[e], wgu.at[slot, :, pl.ds(0, DIM)], w_sem.at[slot, 0]),
                pltpu.make_async_copy(wu_hbm.at[e], wgu.at[slot, :, pl.ds(DIM, DIM)], w_sem.at[slot, 1]),
                pltpu.make_async_copy(wd_hbm.at[e], wd.at[slot], w_sem.at[slot, 2]))

    tokens_in = [pltpu.make_async_copy(xg_hbm.at[h], xgy.at[h], x_sem.at[h]) for h in range(2)]
    for c in tokens_in:
        c.start()
    for e in range(RING):
        for c in weights(jnp.int32(e)):
            c.start()

    local = [jnp.concatenate([meta_ref[n, j:j + 1, :] for n in range(N_DEV)], axis=1) - first.astype(F32) for j in range(TOP_K)]
    gate = jnp.concatenate([meta_ref[n, TOP_K:2 * TOP_K, :] for n in range(N_DEV)], axis=1)
    eid = lax.broadcasted_iota(I32, (LOC, TOK), 0).astype(F32)
    member = jnp.zeros((LOC, TOK), F32)
    for j in range(TOP_K):
        member = member + jnp.where(local[j] == eid, 1.0, 0.0)
    upper = (lax.broadcasted_iota(I32, (BLK, BLK), 0) < lax.broadcasted_iota(I32, (BLK, BLK), 1))
    upper = jnp.where(upper, 1.0, 0.0).astype(BF16)
    parts = [member[:, b * BLK:(b + 1) * BLK] for b in range(N_DEV)]
    before = dot(jnp.concatenate(parts, axis=0).astype(BF16), upper)
    run = jnp.zeros((LOC, 1), F32)
    ranks = []
    for b in range(N_DEV):
        ranks.append(before[b * LOC:(b + 1) * LOC, :] + run)
        run = run + jnp.sum(parts[b], axis=1, keepdims=True)
    rank = jnp.concatenate(ranks, axis=1)
    erow = lax.broadcasted_iota(I32, (LOC, 1), 0)
    off_v = jnp.zeros((LOC, 1), F32)
    off = jnp.int32(0)
    for e in range(LOC):
        cnt = jnp.sum(jnp.where(erow == e, run, 0.0)).astype(I32)
        cnt_ref[e] = cnt
        off_s[e] = off
        off_v = jnp.where(erow == e, off.astype(F32), off_v)
        off = off + ((cnt + 15) // 16) * 16
    n_comb = jnp.maximum((off + COMB - 1) // COMB, 1)
    place = rank + off_v
    for j in range(TOP_K):
        mine = jnp.full((1, TOK), -1.0, F32)
        for e in range(LOC):
            mine = jnp.where(local[j] == float(e), place[e:e + 1, :], mine)
        pos[j:j + 1, :] = mine
    ids = jnp.concatenate(local, axis=0)
    gap = jnp.zeros((TOP_K, TOK), F32)
    slots = jnp.concatenate([*three_parts(gate), gap, ids, ids, ids, gap, pos[0:TOP_K, :], jnp.zeros((BLK - 36, TOK), F32)], axis=0)
    for b in range(N_DEV):
        turned = slots[:, b * BLK:(b + 1) * BLK].T
        pos_t[b * BLK:(b + 1) * BLK, :] = turned
        mt[b * BLK:(b + 1) * BLK, :] = turned.astype(BF16)

    sy[...] = jnp.zeros_like(sy)
    sdx[...] = jnp.zeros_like(sdx)
    dacc[...] = jnp.zeros_like(dacc)
    for c in tokens_in:
        c.wait()

    def gather(i, carry):
        r0 = pl.multiple_of(i * GATHER, GATHER)
        rid = (r0 + lax.broadcasted_iota(I32, (GATHER, 1), 0)).astype(F32)
        here = pl.ds(r0, GATHER)
        picks = []
        for kb in range(TOK // 256):
            lanes = slice(kb * 256, (kb + 1) * 256)
            hit = None
            for j in range(TOP_K):
                m = pos[j:j + 1, lanes] == rid
                hit = m if hit is None else hit | m
            picks.append(jnp.where(hit, 1.0, 0.0).astype(BF16))
        pick = jnp.concatenate(picks, axis=1)
        xs[here, :] = dot(pick, xgy[0]).astype(BF16)
        gys[here, :] = dot(pick, xgy[1]).astype(BF16)
        mrow[here, :] = dot(pick, mt[...]).astype(BF16)
        os_[here, :] = jnp.zeros((GATHER, DIM), BF16)
        ps[here, :] = jnp.zeros((GATHER, DIM + BLK), BF16)
        gcol[here, :] = jnp.zeros((GATHER, 1), F32)
        return carry

    lax.fori_loop(0, 2 * n_comb, gather, 0)

    def chunks(size, items, left=None):
        lane = lax.broadcasted_iota(I32, (size, BLK), 1)
        heres = [pl.ds(pl.multiple_of(base, 16), size) for _, base, _, _ in items]
        xv = [xs[h, :] for h in heres]
        uv = [dot(x, wgu[it[2]]) for x, it in zip(xv, items)]
        gy = [gys[h, :].astype(F32) for h in heres]
        ms = [mrow[h, :].astype(F32) for h in heres]
        match = [(lane < 3 * TOP_K) & (pltpu.roll(m, BLK - 16, 1) == it[0].astype(F32)) for m, it in zip(ms, items)]
        g = [jnp.sum(jnp.where(k, m, 0.0), axis=1, keepdims=True) for k, m in zip(match, ms)]
        q = [(a * b).astype(BF16) for a, b in zip(g, gy)]
        r = [dot(a, wd[it[2]], ((1,), (1,))) for a, it in zip(q, items)]
        u = [a[:, :DIM].astype(BF16).astype(F32) for a in uv]
        v = [a[:, DIM:].astype(BF16).astype(F32) for a in uv]
        s = [jax.nn.sigmoid(a) for a in u]
        act = [(a * b * c).astype(BF16) for a, b, c in zip(u, s, v)]
        o = [dot(a, wd[it[2]]).astype(BF16) for a, it in zip(act, items)]
        dv = [(a * b * c).astype(BF16) for a, b, c in zip(r, u, s)]
        du = [(a * b * c * (1.0 + d * (1.0 - c))).astype(BF16) for a, b, c, d in zip(r, v, s, u)]
        duv = [jnp.concatenate([a, b], axis=1) for a, b in zip(du, dv)]
        p = [dot(a, wgu[it[2]], ((1,), (1,))).astype(BF16) for a, it in zip(duv, items)]
        for i, h in enumerate(heres):
            dgate = jnp.sum(gy[i] * o[i].astype(F32), axis=1, keepdims=True)
            hi, mid, low = three_parts(dgate)
            spread = jnp.where(lane < TOP_K, hi, jnp.where(lane < 2 * TOP_K, mid, low))
            pd = jnp.concatenate([p[i], jnp.where(match[i], spread, 0.0).astype(BF16)], axis=1)
            if left is None:
                os_[h, :] = o[i]
                ps[h, :] = pd
                gcol[h, :] = g[i]
            else:
                keep = lax.broadcasted_iota(I32, (size, 1), 0) < left
                os_[h, :] = jnp.where(keep, o[i].astype(F32), os_[h, :].astype(F32)).astype(BF16)
                ps[h, :] = jnp.where(keep, pd.astype(F32), ps[h, :].astype(F32)).astype(BF16)
                gcol[h, :] = jnp.where(keep, g[i], gcol[h, :])
            stage = items[i][3]
            stage[:, 0:DIM] = xv[i]
            stage[:, DIM:2 * DIM] = act[i]
            stage[:, 2 * DIM:3 * DIM] = q[i]
            stage[:, 3 * DIM:5 * DIM] = duv[i]

    def small_out(e):
        buf = lax.rem(e, 4)
        return pltpu.make_async_copy(stage_s.at[buf], rows_hbm.at[e, pl.ds(0, SMALL)], s_sem.at[buf])

    def big_out(e, b):
        return pltpu.make_async_copy(stage_b, rows_hbm.at[e, pl.ds(pl.multiple_of(SMALL + b * BIG, 32), BIG)], b_sem)

    def pair(i, sent):
        both = [2 * i, 2 * i + 1]
        for e in both:
            for c in weights(e):
                c.wait()

        @pl.when(i >= 2)
        def _():
            for e in both:
                small_out(e - 4).wait()

        chunks(SMALL, [(e, off_s[e], lax.rem(e, RING), stage_s.at[lax.rem(e, 4)]) for e in both])
        for e in both:
            small_out(e).start()
        for e in both:
            def big(b, n, e=e):
                @pl.when(n > 0)
                def _():
                    big_out(e, b).wait()

                base = SMALL + b * BIG
                chunks(BIG, [(e, off_s[e] + base, lax.rem(e, RING), stage_b)], cnt_ref[e] - base)
                big_out(e, b).start()
                return n + 1

            sent = lax.fori_loop(0, (jnp.maximum(cnt_ref[e] - SMALL, 0) + BIG - 1) // BIG, big, sent)

        @pl.when(i + 2 < LOC // 2)
        def _():
            for e in both:
                for c in weights(e + RING):
                    c.start()

        return sent

    sent = lax.fori_loop(0, LOC // 2, pair, jnp.int32(0))
    for e in range(4):
        small_out(jnp.int32(e)).wait()

    @pl.when(sent > 0)
    def _():
        big_out(jnp.int32(0), 0).wait()

    def leave(n, start):
        r, c, k = n // 4, (n // 2) % 2, n % 2
        dr, dc = lax.rem(row + r, 2), lax.rem(col + c, 2)
        for far in range(2):
            ys, dxs = (keep_y, keep_dx) if far == 0 else (send_y, send_dx)

            @pl.when(lax.rem(core + k, 2) == far)
            def _():
                pltpu.make_async_copy(sy.at[n], ys.at[dc * 2 + dr], out_sem.at[n, 0]).start()
                pltpu.make_async_copy(sdx.at[n], dxs.at[dr * 2 + dc], out_sem.at[n, 1]).start()

    def combine(i, last):
        r0 = pl.multiple_of(i * COMB, COMB)
        here = pl.ds(r0, COMB)
        hi, mid, low = three_parts(gcol[here, :] * os_[here, :].astype(F32))
        tri[0:COMB, :] = hi.astype(BF16)
        tri[COMB:2 * COMB, :] = mid.astype(BF16)
        tri[2 * COMB:, :] = low.astype(BF16)
        rid = (r0 + lax.broadcasted_iota(I32, (1, COMB), 1)).astype(F32)
        for t in range(TOK // 256):
            toks = slice(t * 256, (t + 1) * 256)
            hit = None
            for j in range(TOP_K):
                m = pos_t[toks, 32 + j:33 + j] == rid
                hit = m if hit is None else hit | m
            pick = jnp.where(hit, 1.0, 0.0).astype(BF16)
            yb = dot(jnp.concatenate([pick] * 3, axis=1), tri[...])
            db = dot(pick, ps[here, :])
            for k in range(2):
                n = 2 * t + k
                half = slice(k * BLK, (k + 1) * BLK)
                sy[n, 0:BLK, :] += yb[half]
                sdx[n, :, :] += db[half, :DIM]
                dacc[n, :, :] += db[half, DIM:]
                if last:
                    dgt = dacc[n, :, :].T
                    sy[n, BLK:BLK + TOP_K, 0:BLK] = (dgt[0:TOP_K] + dgt[TOP_K:2 * TOP_K]) + dgt[2 * TOP_K:3 * TOP_K]
                    leave(n, True)

    def combine_step(i, carry):
        combine(i, False)
        return carry

    lax.fori_loop(0, n_comb - 1, combine_step, 0)
    combine(n_comb - 1, True)
    for n in range(N_DEV):
        pltpu.make_async_copy(sy.at[n], keep_y.at[0], out_sem.at[n, 0]).wait()
        pltpu.make_async_copy(sdx.at[n], keep_dx.at[0], out_sem.at[n, 1]).wait()


def run_experts(meta_all, xg, w_gate, w_up, w_down):
    vmem = pl.BlockSpec(memory_space=pltpu.VMEM)
    hbm = pl.BlockSpec(memory_space=pl.ANY)
    y_sum = jax.ShapeDtypeStruct((4, BLK + 8, DIM), F32)
    dx_sum = jax.ShapeDtypeStruct((4, BLK, DIM), F32)
    return pl.pallas_call(
        expert_kernel,
        out_shape=(y_sum, y_sum, dx_sum, dx_sum, jax.ShapeDtypeStruct((LOC, SLAB, 5 * DIM), BF16), jax.ShapeDtypeStruct((LOC,), I32)),
        in_specs=[vmem, hbm, hbm, hbm, hbm],
        out_specs=(hbm, hbm, hbm, hbm, hbm, pl.BlockSpec(memory_space=pltpu.SMEM)),
        scratch_shapes=[
            pltpu.VMEM((2, TOK, DIM), BF16), pltpu.VMEM((TOK, BLK), BF16),
            pltpu.VMEM((RING, DIM, 2 * DIM), BF16), pltpu.VMEM((RING, DIM, DIM), BF16),
            pltpu.VMEM((ROWS, DIM), BF16), pltpu.VMEM((ROWS, DIM), BF16), pltpu.VMEM((ROWS, BLK), BF16),
            pltpu.VMEM((ROWS, DIM), BF16), pltpu.VMEM((ROWS, DIM + BLK), BF16), pltpu.VMEM((ROWS, 1), F32),
            pltpu.VMEM((8, TOK), F32), pltpu.VMEM((TOK, BLK), F32), pltpu.VMEM((3 * COMB, DIM), BF16),
            pltpu.VMEM((N_DEV, BLK + 8, DIM), F32), pltpu.VMEM((N_DEV, BLK, DIM), F32), pltpu.VMEM((N_DEV, BLK, BLK), F32),
            pltpu.SMEM((LOC,), I32),
            pltpu.VMEM((4, SMALL, 5 * DIM), BF16), pltpu.VMEM((BIG, 5 * DIM), BF16),
            pltpu.SemaphoreType.DMA((2,)), pltpu.SemaphoreType.DMA((RING, 3)), pltpu.SemaphoreType.DMA((4,)), pltpu.SemaphoreType.DMA,
            pltpu.SemaphoreType.DMA((N_DEV, 2)),
        ],
        compiler_params=pltpu.CompilerParams(vmem_limit_bytes=VMEM_MAX),
        cost_estimate=pl.CostEstimate(flops=6_000_000_000, bytes_accessed=60_000_000, transcendentals=0),
        name="expert_rows",
    )(meta_all, xg, w_gate, w_up, w_down)


def wgrad_kernel(lo, hi, n_alias, cnt_ref, rows_hbm, *refs):
    gg_hbm, gu_hbm, gd_hbm = refs[n_alias:n_alias + 3]
    small, big, out_gu, out_d, r_sem, b_sem, o_sem = refs[n_alias + 3:]

    def rows_in(i):
        return pltpu.make_async_copy(rows_hbm.at[lo + i, pl.ds(0, SMALL)], small.at[lax.rem(i, 2)], r_sem.at[lax.rem(i, 2)])

    def piece_in(i, b):
        return pltpu.make_async_copy(rows_hbm.at[lo + i, pl.ds(pl.multiple_of(b * PIECE, PIECE), PIECE)], big.at[lax.rem(i, 2)], b_sem.at[lax.rem(i, 2)])

    def fetch(i):
        many = cnt_ref[lo + i] > SMALL

        @pl.when(many)
        def _():
            piece_in(i, 0).start()

        @pl.when(jnp.logical_not(many))
        def _():
            rows_in(i).start()

    def results(i):
        slot, e = lax.rem(i, 2), lo + i
        return (pltpu.make_async_copy(out_gu.at[slot, :, pl.ds(0, DIM)], gg_hbm.at[e], o_sem.at[slot, 0]),
                pltpu.make_async_copy(out_gu.at[slot, :, pl.ds(DIM, DIM)], gu_hbm.at[e], o_sem.at[slot, 1]),
                pltpu.make_async_copy(out_d.at[slot], gd_hbm.at[e], o_sem.at[slot, 2]))

    def products(ref, size, left):
        keep = lax.broadcasted_iota(I32, (size, 1), 0) < left
        part = lambda a, b: jnp.where(keep, ref[:, a * DIM:b * DIM].astype(F32), 0.0).astype(BF16)
        x, a, q, duv = part(0, 1), part(1, 2), part(2, 3), part(3, 5)
        return dot(x, duv, ((0,), (0,))), dot(a, q, ((0,), (0,)))

    fetch(jnp.int32(0))

    def expert(i, carry):
        slot = lax.rem(i, 2)
        cnt = cnt_ref[lo + i]

        @pl.when(i + 1 < hi - lo)
        def _():
            fetch(i + 1)

        @pl.when(i >= 2)
        def _():
            for c in results(i - 2):
                c.wait()

        @pl.when(cnt <= SMALL)
        def _():
            rows_in(i).wait()
            g1, g2 = products(small.at[slot], SMALL, cnt)
            out_gu[slot] = g1
            out_d[slot] = g2

        @pl.when(cnt > SMALL)
        def _():
            piece_in(i, 0).wait()
            g1, g2 = products(big.at[slot], PIECE, cnt)
            out_gu[slot] = g1
            out_d[slot] = g2

            def more(b, c2):
                piece_in(i, b).start()
                piece_in(i, b).wait()
                g1, g2 = products(big.at[slot], PIECE, cnt - b * PIECE)
                out_gu[slot] += g1
                out_d[slot] += g2
                return c2

            lax.fori_loop(1, (cnt + PIECE - 1) // PIECE, more, 0)

        for c in results(i):
            c.start()
        return carry

    lax.fori_loop(0, hi - lo, expert, 0)
    for i in (hi - lo - 2, hi - lo - 1):
        for c in results(jnp.int32(i)):
            c.wait()


def weight_grads(lo, hi, cnt, rows, earlier=()):
    hbm = pl.BlockSpec(memory_space=pl.ANY)
    out = jax.ShapeDtypeStruct((LOC, DIM, DIM), F32)
    return pl.pallas_call(
        functools.partial(wgrad_kernel, lo, hi, len(earlier)),
        out_shape=(out, out, out),
        in_specs=[pl.BlockSpec(memory_space=pltpu.SMEM), hbm] + [hbm] * len(earlier),
        out_specs=(hbm, hbm, hbm),
        input_output_aliases={2 + i: i for i in range(len(earlier))},
        scratch_shapes=[
            pltpu.VMEM((2, SMALL, 5 * DIM), BF16), pltpu.VMEM((2, PIECE, 5 * DIM), BF16),
            pltpu.VMEM((2, DIM, 2 * DIM), F32), pltpu.VMEM((2, DIM, DIM), F32),
            pltpu.SemaphoreType.DMA((2,)), pltpu.SemaphoreType.DMA((2,)), pltpu.SemaphoreType.DMA((2, 3)),
        ],
        compiler_params=pltpu.CompilerParams(vmem_limit_bytes=36 * 1024 * 1024),
        cost_estimate=pl.CostEstimate(flops=(hi - lo) * 400_000_000, bytes_accessed=(hi - lo) * 5_000_000, transcendentals=0),
        name="weight_grads",
    )(cnt, rows, *earlier)


def solution(mesh):
    tok_spec = P(None, ALL_AXES, None)
    w_spec = P(ALL_AXES, None, None)

    def swap(value, axis):
        return lax.ppermute(value, axis, [(0, 1), (1, 0)])

    def moe_layer(x, route_idx, gates, w_gate, w_up, w_down, grad_y):
        tok_dev = x.shape[1]
        flat = lambda a: a.reshape(2 * tok_dev, -1)
        turn = lambda a: jnp.transpose(a, (0, 2, 1))
        xg, meta_all = all_gather_tokens(flat(x), flat(grad_y), turn(route_idx), turn(gates))
        keep_y, send_y, keep_dx, send_dx, rows, cnt = run_experts(meta_all, xg.reshape(2, TOK, DIM), w_gate, w_up, w_down)
        chip_y = keep_y + swap(send_y, "core")
        chip_dx = keep_dx + swap(send_dx, "core")
        y_in = swap(chip_y[2:], "col")
        dx_in = swap(chip_dx[2:], "row")
        early = weight_grads(0, 10, cnt, rows)
        y_far = swap(chip_y[1] + y_in[1], "row")
        dx_far = swap(chip_dx[1] + dx_in[1], "col")
        g_gate, g_up, g_down = weight_grads(10, LOC, cnt, rows, early)
        y_sum = chip_y[0] + y_in[0] + y_far
        dx_sum = chip_dx[0] + dx_in[0] + dx_far
        y = y_sum[:BLK].astype(BF16).reshape(x.shape)
        dx = dx_sum.astype(BF16).reshape(x.shape)
        dg = turn(jnp.stack([y_sum[BLK:BLK + TOP_K, m * tok_dev:(m + 1) * tok_dev] for m in range(2)]))
        return y, dx, dg, g_gate, g_up, g_down

    return jax.shard_map(moe_layer, mesh=mesh, in_specs=(tok_spec, tok_spec, tok_spec, w_spec, w_spec, w_spec, tok_spec), out_specs=(tok_spec, tok_spec, tok_spec, w_spec, w_spec, w_spec), check_vma=False)
```

```python
import functools

import jax
import jax.numpy as jnp
from jax import lax
from jax.experimental import pallas as pl
from jax.experimental.pallas import tpu as pltpu
from jax.sharding import PartitionSpec as P

GROUP_AXES = ("row", "col", "core")
ALL_AXES = ("rep", "row", "col", "core")
MESH = pl.DeviceIdType.MESH
F32, BF16, I32 = jnp.float32, jnp.bfloat16, jnp.int32

N_DEV = 8
BLK = 128
TOK = N_DEV * BLK
TOP_K = 4
LOC = 16
DIM = 640
GATHER = 128
COMB = 256
SMALL, BIG = 32, 256
ROWS = 4640
SLAB = 640
RING = 4
PIECE = 288
VMEM_MAX = 67043328


def dot(a, b, dims=((1,), (0,))):
    return lax.dot_general(a, b, (dims, ((), ())), preferred_element_type=F32)


def gather_kernel(x_hbm, gy_hbm, route_ref, gate_ref, xg_hbm, mall_ref, land, own_meta, in_sem, out_sem, meta_sem, send_sem, recv_sem):
    row, col, core = (lax.axis_index(a) for a in GROUP_AXES)
    sib = {"row": row, "col": col, "core": 1 - core}
    xn = {"row": row, "col": 1 - col, "core": core}
    yn = {"row": 1 - row, "col": col, "core": core}

    def index(r, c):
        return (r * 2 + c) * 2 + core

    blocks = {"own": index(row, col), "xn": index(row, 1 - col), "yn": index(1 - row, col), "diag": index(1 - row, 1 - col)}
    pair = {k: b + 1 - 2 * core for k, b in blocks.items()}
    pieces = ("x", "gy", "meta")

    def place(piece, blk):
        if piece == "meta":
            return mall_ref.at[blk]
        return land.at[0 if piece == "x" else 1, blk]

    loads = [pltpu.make_async_copy(x_hbm, place("x", blocks["own"]), in_sem.at[0]),
             pltpu.make_async_copy(gy_hbm, place("gy", blocks["own"]), in_sem.at[1])]
    for c in loads:
        c.start()
    own_meta[0:TOP_K, :] = jnp.concatenate([route_ref[0], route_ref[1]], axis=1).astype(F32)
    own_meta[TOP_K:2 * TOP_K, :] = jnp.concatenate([gate_ref[0], gate_ref[1]], axis=1)

    barrier = pltpu.get_barrier_semaphore()
    for peer in (sib, xn, yn):
        pl.semaphore_signal(barrier, inc=1, device_id=peer, device_id_type=MESH)
    pl.semaphore_wait(barrier, 3)

    meta_copy = pltpu.make_async_copy(own_meta, place("meta", blocks["own"]), meta_sem)
    meta_copy.start()

    names = [("x", "own", p) for p in pieces] + [("y", "own", p) for p in pieces]
    names += [("x", "yn", "gy"), ("y", "xn", "x"), ("y", "xn", "meta")]
    names += [("s", b, p) for b in ("own", "xn", "yn", "diag") for p in pieces]
    number = {n: i for i, n in enumerate(names)}
    peer_of = {"x": xn, "y": yn, "s": sib}

    def copy(name):
        link, b, p = name
        i = number[name]
        src = own_meta if b == "own" and p == "meta" else place(p, blocks[b])
        return pltpu.make_async_remote_copy(
            src_ref=src, dst_ref=place(p, blocks[b]), send_sem=send_sem.at[i], recv_sem=recv_sem.at[i],
            device_id=peer_of[link], device_id_type=MESH)

    copies = {n: copy(n) for n in names}
    stores = []

    def store(p, blk):
        half = 0 if p == "x" else 1
        stores.append(pltpu.make_async_copy(land.at[half, blk], xg_hbm.at[half, blk], out_sem.at[len(stores)]))
        stores[-1].start()

    copies[("x", "own", "meta")].start()
    copies[("y", "own", "meta")].start()
    copies[("s", "own", "meta")].start()
    loads[0].wait()
    copies[("x", "own", "x")].start()
    loads[1].wait()
    for n in (("y", "own", "gy"), ("x", "own", "gy"), ("y", "own", "x"), ("s", "own", "x"), ("s", "own", "gy")):
        copies[n].start()
    store("x", blocks["own"])
    store("gy", blocks["own"])

    def arrived(link, b, p, onward, blk):
        copies[(link, b, p)].wait_recv()
        for n in onward:
            copies[n].start()
        if p != "meta":
            store(p, blk)

    arrived("x", "own", "meta", [("y", "xn", "meta"), ("s", "xn", "meta")], None)
    arrived("y", "own", "meta", [("s", "yn", "meta")], None)
    arrived("x", "own", "x", [("y", "xn", "x"), ("s", "xn", "x")], blocks["xn"])
    arrived("y", "own", "gy", [("x", "yn", "gy"), ("s", "yn", "gy")], blocks["yn"])
    arrived("s", "own", "x", [], pair["own"])
    arrived("s", "own", "gy", [], pair["own"])
    arrived("s", "xn", "x", [], pair["xn"])
    arrived("s", "yn", "gy", [], pair["yn"])
    arrived("x", "own", "gy", [("s", "xn", "gy")], blocks["xn"])
    arrived("y", "own", "x", [("s", "yn", "x")], blocks["yn"])
    arrived("y", "xn", "meta", [("s", "diag", "meta")], None)
    arrived("s", "xn", "gy", [], pair["xn"])
    arrived("s", "yn", "x", [], pair["yn"])
    arrived("y", "xn", "x", [("s", "diag", "x")], blocks["diag"])
    arrived("x", "yn", "gy", [("s", "diag", "gy")], blocks["diag"])
    for b in ("own", "xn", "yn", "diag"):
        arrived("s", b, "meta", [], None)
    arrived("s", "diag", "x", [], pair["diag"])
    arrived("s", "diag", "gy", [], pair["diag"])
    for n in names:
        copies[n].wait_send()
    meta_copy.wait()
    for c in stores:
        c.wait()


def all_gather_tokens(x_loc, gy_loc, route, gates):
    n_copies = 21
    vmem = pl.BlockSpec(memory_space=pltpu.VMEM)
    hbm = pl.BlockSpec(memory_space=pl.ANY)
    return pl.pallas_call(
        gather_kernel,
        out_shape=(jax.ShapeDtypeStruct((2, N_DEV, BLK, DIM), BF16), jax.ShapeDtypeStruct((N_DEV, 8, BLK), F32)),
        in_specs=[hbm, hbm, vmem, vmem],
        out_specs=(hbm, vmem),
        scratch_shapes=[pltpu.VMEM((2, N_DEV, BLK, DIM), BF16), pltpu.VMEM((8, BLK), F32), pltpu.SemaphoreType.DMA((2,)),
                        pltpu.SemaphoreType.DMA((16,)), pltpu.SemaphoreType.DMA,
                        pltpu.SemaphoreType.DMA((n_copies,)), pltpu.SemaphoreType.DMA((n_copies,))],
        compiler_params=pltpu.CompilerParams(collective_id=0, has_side_effects=True),
        name="token_gather",
    )(x_loc, gy_loc, route, gates)


def three_parts(value):
    hi = value.astype(BF16).astype(F32)
    mid = (value - hi).astype(BF16).astype(F32)
    return hi, mid, value - hi - mid


def expert_kernel(meta_ref, xg_hbm, wg_hbm, wu_hbm, wd_hbm, near_k, near_s, far_k, far_s, rows_hbm, cnt_ref,
                  xgy, mt, wgu, wd, xs, gys, mrow, os_, ps, gcol, pos, pos_t, tri, sy, sdx, dacc, off_s, stage_s, stage_b,
                  x_sem, w_sem, s_sem, b_sem, out_sem):
    row, col, core = (lax.axis_index(a) for a in GROUP_AXES)
    first = ((row * 2 + col) * 2 + core) * LOC
    sums = ((near_k, near_s), (far_k, far_s))

    def weights(e):
        slot, wide = lax.rem(e, RING), lax.rem(e, RING + 2)
        return (pltpu.make_async_copy(wg_hbm.at[e], wgu.at[wide, :, pl.ds(0, DIM)], w_sem.at[slot, 0]),
                pltpu.make_async_copy(wu_hbm.at[e], wgu.at[wide, :, pl.ds(DIM, DIM)], w_sem.at[slot, 1]),
                pltpu.make_async_copy(wd_hbm.at[e], wd.at[slot], w_sem.at[slot, 2]))

    tokens_in = [pltpu.make_async_copy(xg_hbm.at[h], xgy.at[h], x_sem.at[h]) for h in range(2)]
    for c in tokens_in:
        c.start()
    for e in range(RING):
        for c in weights(jnp.int32(e)):
            c.start()

    local = [jnp.concatenate([meta_ref[n, j:j + 1, :] for n in range(N_DEV)], axis=1) - first.astype(F32) for j in range(TOP_K)]
    gate = jnp.concatenate([meta_ref[n, TOP_K:2 * TOP_K, :] for n in range(N_DEV)], axis=1)
    eid = lax.broadcasted_iota(I32, (LOC, TOK), 0).astype(F32)
    member = jnp.zeros((LOC, TOK), F32)
    for j in range(TOP_K):
        member = member + jnp.where(local[j] == eid, 1.0, 0.0)
    upper = (lax.broadcasted_iota(I32, (BLK, BLK), 0) < lax.broadcasted_iota(I32, (BLK, BLK), 1))
    upper = jnp.where(upper, 1.0, 0.0).astype(BF16)
    parts = [member[:, b * BLK:(b + 1) * BLK] for b in range(N_DEV)]
    before = dot(jnp.concatenate(parts, axis=0).astype(BF16), upper)
    run = jnp.zeros((LOC, 1), F32)
    ranks = []
    for b in range(N_DEV):
        ranks.append(before[b * LOC:(b + 1) * LOC, :] + run)
        run = run + jnp.sum(parts[b], axis=1, keepdims=True)
    rank = jnp.concatenate(ranks, axis=1)
    erow = lax.broadcasted_iota(I32, (LOC, 1), 0)
    off_v = jnp.zeros((LOC, 1), F32)
    off = jnp.int32(0)
    for e in range(LOC):
        cnt = jnp.sum(jnp.where(erow == e, run, 0.0)).astype(I32)
        cnt_ref[e] = cnt
        off_s[e] = off
        off_v = jnp.where(erow == e, off.astype(F32), off_v)
        off = off + ((cnt + 15) // 16) * 16
    n_comb = jnp.maximum((off + COMB - 1) // COMB, 1)
    place = rank + off_v
    for j in range(TOP_K):
        mine = jnp.full((1, TOK), -1.0, F32)
        for e in range(LOC):
            mine = jnp.where(local[j] == float(e), place[e:e + 1, :], mine)
        pos[j:j + 1, :] = mine
    ids = jnp.concatenate(local, axis=0)
    gap = jnp.zeros((TOP_K, TOK), F32)
    slots = jnp.concatenate([*three_parts(gate), gap, ids, ids, ids, gap, pos[0:TOP_K, :], jnp.zeros((BLK - 36, TOK), F32)], axis=0)
    for b in range(N_DEV):
        turned = slots[:, b * BLK:(b + 1) * BLK].T
        pos_t[b * BLK:(b + 1) * BLK, :] = turned
        mt[b * BLK:(b + 1) * BLK, :] = turned.astype(BF16)

    sy[...] = jnp.zeros_like(sy)
    sdx[...] = jnp.zeros_like(sdx)
    dacc[...] = jnp.zeros_like(dacc)
    for c in tokens_in:
        c.wait()

    def gather(i, carry):
        r0 = pl.multiple_of(i * GATHER, GATHER)
        rid = (r0 + lax.broadcasted_iota(I32, (GATHER, 1), 0)).astype(F32)
        here = pl.ds(r0, GATHER)
        picks = []
        for kb in range(TOK // 256):
            lanes = slice(kb * 256, (kb + 1) * 256)
            hit = None
            for j in range(TOP_K):
                m = pos[j:j + 1, lanes] == rid
                hit = m if hit is None else hit | m
            picks.append(jnp.where(hit, 1.0, 0.0).astype(BF16))
        pick = jnp.concatenate(picks, axis=1)
        xs[here, :] = dot(pick, xgy[0]).astype(BF16)
        gys[here, :] = dot(pick, xgy[1]).astype(BF16)
        mrow[here, :] = dot(pick, mt[...]).astype(BF16)
        os_[here, :] = jnp.zeros((GATHER, DIM), BF16)
        ps[here, :] = jnp.zeros((GATHER, DIM + BLK), BF16)
        gcol[here, :] = jnp.zeros((GATHER, 1), F32)
        return carry

    lax.fori_loop(0, 2 * n_comb, gather, 0)

    def chunks(size, items, left=None, between=iter(())):
        lane = lax.broadcasted_iota(I32, (size, BLK), 1)
        heres = [pl.ds(pl.multiple_of(it[1], 16), size) for it in items]
        xv = [xs[h, :] for h in heres]
        credit = [0.0]

        def tiled(width, cost, product):
            tiles = []
            for n in range(0, width, 256):
                m = min(n + 256, width)
                tiles.append(product(n, m))
                credit[0] += cost * (m - n) / 256
                while credit[0] >= 1.0:
                    next(between, None)
                    credit[0] -= 1.0
            return jnp.concatenate(tiles, axis=1)

        uv = [tiled(2 * DIM, 0.36, lambda n, m, x=x, it=it: dot(x, wgu[it[3], :, n:m])) for x, it in zip(xv, items)]
        gy = [gys[h, :].astype(F32) for h in heres]
        ms = [mrow[h, :].astype(F32) for h in heres]
        match = [(lane < 3 * TOP_K) & (pltpu.roll(m, BLK - 16, 1) == it[0].astype(F32)) for m, it in zip(ms, items)]
        g = [jnp.sum(jnp.where(k, m, 0.0), axis=1, keepdims=True) for k, m in zip(match, ms)]
        q = [(a * b).astype(BF16) for a, b in zip(g, gy)]
        r = [tiled(DIM, 0.85, lambda n, m, a=a, it=it: dot(a, wd[it[2], n:m, :], ((1,), (1,)))) for a, it in zip(q, items)]
        u = [a[:, :DIM].astype(BF16).astype(F32) for a in uv]
        v = [a[:, DIM:].astype(BF16).astype(F32) for a in uv]
        s = [jax.nn.sigmoid(a) for a in u]
        act = [(a * b * c).astype(BF16) for a, b, c in zip(u, s, v)]
        o = [tiled(DIM, 0.43, lambda n, m, a=a, it=it: dot(a, wd[it[2], :, n:m])).astype(BF16) for a, it in zip(act, items)]
        dv = [(a * b * c).astype(BF16) for a, b, c in zip(r, u, s)]
        du = [(a * b * c * (1.0 + d * (1.0 - c))).astype(BF16) for a, b, c, d in zip(r, v, s, u)]
        duv = [jnp.concatenate([a, b], axis=1) for a, b in zip(du, dv)]
        for i, h in enumerate(heres):
            dgate = jnp.sum(gy[i] * o[i].astype(F32), axis=1, keepdims=True)
            hi, mid, low = three_parts(dgate)
            spread = jnp.where(lane < TOP_K, hi, jnp.where(lane < 2 * TOP_K, mid, low))
            dgs = jnp.where(match[i], spread, 0.0).astype(BF16)
            if left is None:
                os_[h, :] = o[i]
                ps[h, DIM:] = dgs
                gcol[h, :] = g[i]
            else:
                p = dot(duv[i], wgu[items[i][3]], ((1,), (1,))).astype(BF16)
                pd = jnp.concatenate([p, dgs], axis=1)
                keep = lax.broadcasted_iota(I32, (size, 1), 0) < left
                os_[h, :] = jnp.where(keep, o[i].astype(F32), os_[h, :].astype(F32)).astype(BF16)
                ps[h, :] = jnp.where(keep, pd.astype(F32), ps[h, :].astype(F32)).astype(BF16)
                gcol[h, :] = jnp.where(keep, g[i], gcol[h, :])
            stage = items[i][4]
            stage[:, 0:DIM] = xv[i]
            stage[:, DIM:2 * DIM] = act[i]
            stage[:, 2 * DIM:3 * DIM] = q[i]
            stage[:, 3 * DIM:5 * DIM] = duv[i]

    def input_grads(items):
        for _, base, _, wide, stage in items:
            duv = stage[:, 3 * DIM:5 * DIM]
            for d in range(0, DIM, 128):
                p = dot(wgu[wide, d:d + 128, :], duv, ((1,), (1,))).T.astype(BF16)
                ps[pl.ds(pl.multiple_of(base, 16), SMALL), d:d + 128] = p
                yield

    def small(e):
        return (e, off_s[e], lax.rem(e, RING), lax.rem(e, RING + 2), stage_s.at[lax.rem(e, 4)])

    def earlier(e, i):
        before = lax.rem(e + LOC - 2, LOC)
        return (before, jnp.where(i > 0, off_s[before], ROWS - SMALL), 0, lax.rem(e + RING, RING + 2), stage_s.at[lax.rem(e + 2, 4)])

    def small_out(e):
        buf = lax.rem(e, 4)
        return pltpu.make_async_copy(stage_s.at[buf], rows_hbm.at[e, pl.ds(0, SMALL)], s_sem.at[buf])

    def big_out(e, b):
        return pltpu.make_async_copy(stage_b, rows_hbm.at[e, pl.ds(pl.multiple_of(SMALL + b * BIG, 32), BIG)], b_sem)

    def pair(i, sent):
        both = [2 * i, 2 * i + 1]
        for e in both:
            for c in weights(e):
                c.wait()

        @pl.when(i >= 2)
        def _():
            for e in both:
                small_out(e - 4).wait()

        between = input_grads([earlier(e, i) for e in both])
        chunks(SMALL, [small(e) for e in both], between=between)
        for _ in between:
            pass
        for e in both:
            small_out(e).start()
        for e in both:
            def big(b, n, e=e):
                @pl.when(n > 0)
                def _():
                    big_out(e, b).wait()

                base = SMALL + b * BIG
                chunks(BIG, [(e, off_s[e] + base, lax.rem(e, RING), lax.rem(e, RING + 2), stage_b)], cnt_ref[e] - base)
                big_out(e, b).start()
                return n + 1

            sent = lax.fori_loop(0, (jnp.maximum(cnt_ref[e] - SMALL, 0) + BIG - 1) // BIG, big, sent)

        @pl.when(i + 2 < LOC // 2)
        def _():
            for e in both:
                for c in weights(e + RING):
                    c.start()

        return sent

    sent = lax.fori_loop(0, LOC // 2, pair, jnp.int32(0))
    for _ in input_grads([small(jnp.int32(e)) for e in (LOC - 2, LOC - 1)]):
        pass
    for e in range(4):
        small_out(jnp.int32(e)).wait()

    @pl.when(sent > 0)
    def _():
        big_out(jnp.int32(0), 0).wait()

    def leave(n):
        r, c, k = n // 4, (n // 2) % 2, n % 2
        dr, dc, dk = lax.rem(row + r, 2), lax.rem(col + c, 2), lax.rem(core + k, 2)
        for far in range(2):
            for send in range(2):
                @pl.when((dk == send) & (dc == far))
                def _():
                    pltpu.make_async_copy(sy.at[n], sums[far][send].at[dr], out_sem.at[n, 0]).start()

                @pl.when((dk == send) & (dr == far))
                def _():
                    pltpu.make_async_copy(sdx.at[n], sums[far][send].at[2 + dc, pl.ds(0, BLK)], out_sem.at[n, 1]).start()

    def combine(i, last):
        r0 = pl.multiple_of(i * COMB, COMB)
        here = pl.ds(r0, COMB)
        hi, mid, low = three_parts(gcol[here, :] * os_[here, :].astype(F32))
        tri[0:COMB, :] = hi.astype(BF16)
        tri[COMB:2 * COMB, :] = mid.astype(BF16)
        tri[2 * COMB:, :] = low.astype(BF16)
        rid = (r0 + lax.broadcasted_iota(I32, (1, COMB), 1)).astype(F32)
        for t in range(TOK // 256):
            toks = slice(t * 256, (t + 1) * 256)
            hit = None
            for j in range(TOP_K):
                m = pos_t[toks, 32 + j:33 + j] == rid
                hit = m if hit is None else hit | m
            pick = jnp.where(hit, 1.0, 0.0).astype(BF16)
            yb = dot(jnp.concatenate([pick] * 3, axis=1), tri[...])
            db = dot(pick, ps[here, :])
            for k in range(2):
                n = 2 * t + k
                half = slice(k * BLK, (k + 1) * BLK)
                sy[n, 0:BLK, :] += yb[half]
                sdx[n, :, :] += db[half, :DIM]
                dacc[n, :, :] += db[half, DIM:]
                if last:
                    dgt = dacc[n, :, :].T
                    sy[n, BLK:BLK + TOP_K, 0:BLK] = (dgt[0:TOP_K] + dgt[TOP_K:2 * TOP_K]) + dgt[2 * TOP_K:3 * TOP_K]
                    leave(n)

    def combine_step(i, carry):
        combine(i, False)
        return carry

    lax.fori_loop(0, n_comb - 1, combine_step, 0)
    combine(n_comb - 1, True)
    for n in range(N_DEV):
        pltpu.make_async_copy(sy.at[n], near_k.at[0], out_sem.at[n, 0]).wait()
        pltpu.make_async_copy(sdx.at[n], near_k.at[2, pl.ds(0, BLK)], out_sem.at[n, 1]).wait()


def run_experts(meta_all, xg, w_gate, w_up, w_down):
    vmem = pl.BlockSpec(memory_space=pltpu.VMEM)
    hbm = pl.BlockSpec(memory_space=pl.ANY)
    sums = jax.ShapeDtypeStruct((4, BLK + 8, DIM), F32)
    return pl.pallas_call(
        expert_kernel,
        out_shape=(*[sums] * 4, jax.ShapeDtypeStruct((LOC, SLAB, 5 * DIM), BF16), jax.ShapeDtypeStruct((LOC,), I32)),
        in_specs=[vmem, hbm, hbm, hbm, hbm],
        out_specs=(*[hbm] * 5, pl.BlockSpec(memory_space=pltpu.SMEM)),
        scratch_shapes=[
            pltpu.VMEM((2, TOK, DIM), BF16), pltpu.VMEM((TOK, BLK), BF16),
            pltpu.VMEM((RING + 2, DIM, 2 * DIM), BF16), pltpu.VMEM((RING, DIM, DIM), BF16),
            pltpu.VMEM((ROWS, DIM), BF16), pltpu.VMEM((ROWS, DIM), BF16), pltpu.VMEM((ROWS, BLK), BF16),
            pltpu.VMEM((ROWS, DIM), BF16), pltpu.VMEM((ROWS, DIM + BLK), BF16), pltpu.VMEM((ROWS, 1), F32),
            pltpu.VMEM((8, TOK), F32), pltpu.VMEM((TOK, BLK), F32), pltpu.VMEM((3 * COMB, DIM), BF16),
            pltpu.VMEM((N_DEV, BLK + 8, DIM), F32), pltpu.VMEM((N_DEV, BLK, DIM), F32), pltpu.VMEM((N_DEV, BLK, BLK), F32),
            pltpu.SMEM((LOC,), I32),
            pltpu.VMEM((4, SMALL, 5 * DIM), BF16), pltpu.VMEM((BIG, 5 * DIM), BF16),
            pltpu.SemaphoreType.DMA((2,)), pltpu.SemaphoreType.DMA((RING, 3)), pltpu.SemaphoreType.DMA((4,)), pltpu.SemaphoreType.DMA,
            pltpu.SemaphoreType.DMA((N_DEV, 2)),
        ],
        compiler_params=pltpu.CompilerParams(vmem_limit_bytes=VMEM_MAX),
        cost_estimate=pl.CostEstimate(flops=6_000_000_000, bytes_accessed=60_000_000, transcendentals=0),
        name="expert_rows",
    )(meta_all, xg, w_gate, w_up, w_down)


def wgrad_kernel(lo, hi, n_alias, cnt_ref, rows_hbm, *refs):
    gg_hbm, gu_hbm, gd_hbm = refs[n_alias:n_alias + 3]
    small, big, out_gu, out_d, r_sem, b_sem, o_sem = refs[n_alias + 3:]

    def rows_in(i):
        return pltpu.make_async_copy(rows_hbm.at[lo + i, pl.ds(0, SMALL)], small.at[lax.rem(i, 2)], r_sem.at[lax.rem(i, 2)])

    def piece_in(i, b):
        return pltpu.make_async_copy(rows_hbm.at[lo + i, pl.ds(pl.multiple_of(b * PIECE, PIECE), PIECE)], big.at[lax.rem(i, 2)], b_sem.at[lax.rem(i, 2)])

    def fetch(i):
        many = cnt_ref[lo + i] > SMALL

        @pl.when(many)
        def _():
            piece_in(i, 0).start()

        @pl.when(jnp.logical_not(many))
        def _():
            rows_in(i).start()

    def results(i):
        slot, e = lax.rem(i, 2), lo + i
        return (pltpu.make_async_copy(out_gu.at[slot, :, pl.ds(0, DIM)], gg_hbm.at[e], o_sem.at[slot, 0]),
                pltpu.make_async_copy(out_gu.at[slot, :, pl.ds(DIM, DIM)], gu_hbm.at[e], o_sem.at[slot, 1]),
                pltpu.make_async_copy(out_d.at[slot], gd_hbm.at[e], o_sem.at[slot, 2]))

    def products(ref, size, left):
        keep = lax.broadcasted_iota(I32, (size, 1), 0) < left
        part = lambda a, b: jnp.where(keep, ref[:, a * DIM:b * DIM].astype(F32), 0.0).astype(BF16)
        x, a, q, duv = part(0, 1), part(1, 2), part(2, 3), part(3, 5)
        return dot(x, duv, ((0,), (0,))), dot(a, q, ((0,), (0,)))

    fetch(jnp.int32(0))

    def expert(i, carry):
        slot = lax.rem(i, 2)
        cnt = cnt_ref[lo + i]

        @pl.when(i + 1 < hi - lo)
        def _():
            fetch(i + 1)

        @pl.when(i >= 2)
        def _():
            for c in results(i - 2):
                c.wait()

        @pl.when(cnt <= SMALL)
        def _():
            rows_in(i).wait()
            g1, g2 = products(small.at[slot], SMALL, cnt)
            out_gu[slot] = g1
            out_d[slot] = g2

        @pl.when(cnt > SMALL)
        def _():
            piece_in(i, 0).wait()
            g1, g2 = products(big.at[slot], PIECE, cnt)
            out_gu[slot] = g1
            out_d[slot] = g2

            def more(b, c2):
                piece_in(i, b).start()
                piece_in(i, b).wait()
                g1, g2 = products(big.at[slot], PIECE, cnt - b * PIECE)
                out_gu[slot] += g1
                out_d[slot] += g2
                return c2

            lax.fori_loop(1, (cnt + PIECE - 1) // PIECE, more, 0)

        for c in results(i):
            c.start()
        return carry

    lax.fori_loop(0, hi - lo, expert, 0)
    for i in (hi - lo - 2, hi - lo - 1):
        for c in results(jnp.int32(i)):
            c.wait()


def weight_grads(lo, hi, cnt, rows, earlier=()):
    hbm = pl.BlockSpec(memory_space=pl.ANY)
    out = jax.ShapeDtypeStruct((LOC, DIM, DIM), F32)
    return pl.pallas_call(
        functools.partial(wgrad_kernel, lo, hi, len(earlier)),
        out_shape=(out, out, out),
        in_specs=[pl.BlockSpec(memory_space=pltpu.SMEM), hbm] + [hbm] * len(earlier),
        out_specs=(hbm, hbm, hbm),
        input_output_aliases={2 + i: i for i in range(len(earlier))},
        scratch_shapes=[
            pltpu.VMEM((2, SMALL, 5 * DIM), BF16), pltpu.VMEM((2, PIECE, 5 * DIM), BF16),
            pltpu.VMEM((2, DIM, 2 * DIM), F32), pltpu.VMEM((2, DIM, DIM), F32),
            pltpu.SemaphoreType.DMA((2,)), pltpu.SemaphoreType.DMA((2,)), pltpu.SemaphoreType.DMA((2, 3)),
        ],
        compiler_params=pltpu.CompilerParams(vmem_limit_bytes=36 * 1024 * 1024),
        cost_estimate=pl.CostEstimate(flops=(hi - lo) * 400_000_000, bytes_accessed=(hi - lo) * 5_000_000, transcendentals=0),
        name="weight_grads",
    )(cnt, rows, *earlier)


def solution(mesh):
    tok_spec = P(None, ALL_AXES, None)
    w_spec = P(ALL_AXES, None, None)

    def swap(value, axis):
        return lax.ppermute(value, axis, [(0, 1), (1, 0)])

    def moe_layer(x, route_idx, gates, w_gate, w_up, w_down, grad_y):
        tok_dev = x.shape[1]
        flat = lambda a: a.reshape(2 * tok_dev, -1)
        turn = lambda a: jnp.transpose(a, (0, 2, 1))
        xg, meta_all = all_gather_tokens(flat(x), flat(grad_y), turn(route_idx), turn(gates))
        near_k, near_s, far_k, far_s, rows, cnt = run_experts(meta_all, xg.reshape(2, TOK, DIM), w_gate, w_up, w_down)
        far_in = swap(far_s, "core")
        y_in = swap(far_k[:2] + far_in[:2], "col")
        dx_in = swap(far_k[2:, :BLK] + far_in[2:, :BLK], "row")
        near_in = swap(near_s, "core")
        early = weight_grads(0, 10, cnt, rows)
        y_out = near_k[1] + near_in[1] + y_in[1]
        dx_out = near_k[3, :BLK] + near_in[3, :BLK] + dx_in[1]
        y_out, dx_out, early = lax.optimization_barrier((y_out, dx_out, early))
        y_far, dx_far = swap(y_out, "row"), swap(dx_out, "col")
        g_gate, g_up, g_down = weight_grads(10, LOC, cnt, rows, early)
        y = (near_k[0, :BLK] + near_in[0, :BLK] + y_in[0, :BLK] + y_far[:BLK]).astype(BF16).reshape(x.shape)
        dx = (near_k[2, :BLK] + near_in[2, :BLK] + dx_in[0] + dx_far).astype(BF16).reshape(x.shape)
        tail = slice(BLK, BLK + TOP_K)
        dg = near_k[0, tail, :BLK] + near_in[0, tail, :BLK] + y_in[0, tail, :BLK] + y_far[tail, :BLK]
        dg = turn(jnp.stack([dg[:, m * tok_dev:(m + 1) * tok_dev] for m in range(2)]))
        return y, dx, dg, g_gate, g_up, g_down

    return jax.shard_map(moe_layer, mesh=mesh, in_specs=(tok_spec, tok_spec, tok_spec, w_spec, w_spec, w_spec, tok_spec), out_specs=(tok_spec, tok_spec, tok_spec, w_spec, w_spec, w_spec), check_vma=False)
```

```python
import functools

import jax
import jax.numpy as jnp
from jax import lax
from jax.experimental import pallas as pl
from jax.experimental.pallas import tpu as pltpu
from jax.sharding import PartitionSpec as P

GROUP_AXES = ("row", "col", "core")
ALL_AXES = ("rep", "row", "col", "core")
MESH = pl.DeviceIdType.MESH
F32, BF16, I32 = jnp.float32, jnp.bfloat16, jnp.int32

N_DEV = 8
BLK = 128
TOK = N_DEV * BLK
TOP_K = 4
LOC = 16
DIM = 640
GATHER = 256
COMB = 256
SMALL, BIG = 32, 256
ROWS = 4640
SLAB = 640
RING = 4
PIECE = 288
VMEM_MAX = 67043328


def dot(a, b, dims=((1,), (0,))):
    return lax.dot_general(a, b, (dims, ((), ())), preferred_element_type=F32)


def gather_kernel(x_hbm, gy_hbm, route_ref, gate_ref, xg_hbm, mall_ref, land, own_meta, in_sem, out_sem, meta_sem, send_sem, recv_sem):
    row, col, core = (lax.axis_index(a) for a in GROUP_AXES)
    sib = {"row": row, "col": col, "core": 1 - core}
    xn = {"row": row, "col": 1 - col, "core": core}
    yn = {"row": 1 - row, "col": col, "core": core}

    def index(r, c):
        return (r * 2 + c) * 2 + core

    blocks = {"own": index(row, col), "xn": index(row, 1 - col), "yn": index(1 - row, col), "diag": index(1 - row, 1 - col)}
    pair = {k: b + 1 - 2 * core for k, b in blocks.items()}
    pieces = ("x", "gy", "meta")

    def place(piece, blk):
        if piece == "meta":
            return mall_ref.at[blk]
        return land.at[0 if piece == "x" else 1, blk]

    loads = [pltpu.make_async_copy(x_hbm, place("x", blocks["own"]), in_sem.at[0]),
             pltpu.make_async_copy(gy_hbm, place("gy", blocks["own"]), in_sem.at[1])]
    for c in loads:
        c.start()
    own_meta[0:TOP_K, :] = jnp.concatenate([route_ref[0], route_ref[1]], axis=1).astype(F32)
    own_meta[TOP_K:2 * TOP_K, :] = jnp.concatenate([gate_ref[0], gate_ref[1]], axis=1)

    barrier = pltpu.get_barrier_semaphore()
    for peer in (sib, xn, yn):
        pl.semaphore_signal(barrier, inc=1, device_id=peer, device_id_type=MESH)
    pl.semaphore_wait(barrier, 3)

    meta_copy = pltpu.make_async_copy(own_meta, place("meta", blocks["own"]), meta_sem)
    meta_copy.start()

    names = [("x", "own", p) for p in pieces] + [("y", "own", p) for p in pieces]
    names += [("x", "yn", "gy"), ("y", "xn", "x"), ("y", "xn", "meta")]
    names += [("s", b, p) for b in ("own", "xn", "yn", "diag") for p in pieces]
    number = {n: i for i, n in enumerate(names)}
    peer_of = {"x": xn, "y": yn, "s": sib}

    def copy(name):
        link, b, p = name
        i = number[name]
        src = own_meta if b == "own" and p == "meta" else place(p, blocks[b])
        return pltpu.make_async_remote_copy(
            src_ref=src, dst_ref=place(p, blocks[b]), send_sem=send_sem.at[i], recv_sem=recv_sem.at[i],
            device_id=peer_of[link], device_id_type=MESH)

    copies = {n: copy(n) for n in names}
    stores = []

    def store(p, blk):
        half = 0 if p == "x" else 1
        stores.append(pltpu.make_async_copy(land.at[half, blk], xg_hbm.at[half, blk], out_sem.at[len(stores)]))
        stores[-1].start()

    copies[("x", "own", "meta")].start()
    copies[("y", "own", "meta")].start()
    copies[("s", "own", "meta")].start()
    loads[0].wait()
    copies[("x", "own", "x")].start()
    loads[1].wait()
    for n in (("y", "own", "gy"), ("x", "own", "gy"), ("y", "own", "x"), ("s", "own", "x"), ("s", "own", "gy")):
        copies[n].start()
    store("x", blocks["own"])
    store("gy", blocks["own"])

    def arrived(link, b, p, onward, blk):
        copies[(link, b, p)].wait_recv()
        for n in onward:
            copies[n].start()
        if p != "meta":
            store(p, blk)

    arrived("x", "own", "meta", [("y", "xn", "meta"), ("s", "xn", "meta")], None)
    arrived("y", "own", "meta", [("s", "yn", "meta")], None)
    arrived("x", "own", "x", [("y", "xn", "x"), ("s", "xn", "x")], blocks["xn"])
    arrived("y", "own", "gy", [("x", "yn", "gy"), ("s", "yn", "gy")], blocks["yn"])
    arrived("s", "own", "x", [], pair["own"])
    arrived("s", "own", "gy", [], pair["own"])
    arrived("s", "xn", "x", [], pair["xn"])
    arrived("s", "yn", "gy", [], pair["yn"])
    arrived("x", "own", "gy", [("s", "xn", "gy")], blocks["xn"])
    arrived("y", "own", "x", [("s", "yn", "x")], blocks["yn"])
    arrived("y", "xn", "meta", [("s", "diag", "meta")], None)
    arrived("s", "xn", "gy", [], pair["xn"])
    arrived("s", "yn", "x", [], pair["yn"])
    arrived("y", "xn", "x", [("s", "diag", "x")], blocks["diag"])
    arrived("x", "yn", "gy", [("s", "diag", "gy")], blocks["diag"])
    for b in ("own", "xn", "yn", "diag"):
        arrived("s", b, "meta", [], None)
    arrived("s", "diag", "x", [], pair["diag"])
    arrived("s", "diag", "gy", [], pair["diag"])
    for n in names:
        copies[n].wait_send()
    meta_copy.wait()
    for c in stores:
        c.wait()


def all_gather_tokens(x_loc, gy_loc, route, gates):
    n_copies = 21
    vmem = pl.BlockSpec(memory_space=pltpu.VMEM)
    hbm = pl.BlockSpec(memory_space=pl.ANY)
    return pl.pallas_call(
        gather_kernel,
        out_shape=(jax.ShapeDtypeStruct((2, N_DEV, BLK, DIM), BF16), jax.ShapeDtypeStruct((N_DEV, 8, BLK), F32)),
        in_specs=[hbm, hbm, vmem, vmem],
        out_specs=(hbm, vmem),
        scratch_shapes=[pltpu.VMEM((2, N_DEV, BLK, DIM), BF16), pltpu.VMEM((8, BLK), F32), pltpu.SemaphoreType.DMA((2,)),
                        pltpu.SemaphoreType.DMA((16,)), pltpu.SemaphoreType.DMA,
                        pltpu.SemaphoreType.DMA((n_copies,)), pltpu.SemaphoreType.DMA((n_copies,))],
        compiler_params=pltpu.CompilerParams(collective_id=0, has_side_effects=True),
        name="token_gather",
    )(x_loc, gy_loc, route, gates)


def three_parts(value):
    hi = value.astype(BF16).astype(F32)
    mid = (value - hi).astype(BF16).astype(F32)
    return hi, mid, value - hi - mid


def expert_kernel(meta_ref, xg_hbm, wg_hbm, wu_hbm, wd_hbm, near_k, near_s, far_k, far_s, rows_hbm, cnt_ref,
                  xgy, mt, wgu, wd, xs, gys, mrow, os_, ps, gcol, pos, pos_t, tri, sy, sdx, dacc, off_s, stage_s, stage_b,
                  x_sem, w_sem, s_sem, b_sem, out_sem):
    row, col, core = (lax.axis_index(a) for a in GROUP_AXES)
    first = ((row * 2 + col) * 2 + core) * LOC
    sums = ((near_k, near_s), (far_k, far_s))

    def weights(e):
        slot, wide = lax.rem(e, RING), lax.rem(e, RING + 2)
        return (pltpu.make_async_copy(wg_hbm.at[e], wgu.at[wide, :, pl.ds(0, DIM)], w_sem.at[slot, 0]),
                pltpu.make_async_copy(wu_hbm.at[e], wgu.at[wide, :, pl.ds(DIM, DIM)], w_sem.at[slot, 1]),
                pltpu.make_async_copy(wd_hbm.at[e], wd.at[slot], w_sem.at[slot, 2]))

    tokens_in = [pltpu.make_async_copy(xg_hbm.at[h], xgy.at[h], x_sem.at[h]) for h in range(2)]
    for c in tokens_in:
        c.start()
    for e in range(RING):
        for c in weights(jnp.int32(e)):
            c.start()

    local = [jnp.concatenate([meta_ref[n, j:j + 1, :] for n in range(N_DEV)], axis=1) - first.astype(F32) for j in range(TOP_K)]
    gate = jnp.concatenate([meta_ref[n, TOP_K:2 * TOP_K, :] for n in range(N_DEV)], axis=1)
    eid = lax.broadcasted_iota(I32, (LOC, TOK), 0).astype(F32)
    member = jnp.zeros((LOC, TOK), F32)
    for j in range(TOP_K):
        member = member + jnp.where(local[j] == eid, 1.0, 0.0)
    upper = (lax.broadcasted_iota(I32, (BLK, BLK), 0) < lax.broadcasted_iota(I32, (BLK, BLK), 1))
    upper = jnp.where(upper, 1.0, 0.0).astype(BF16)
    parts = [member[:, b * BLK:(b + 1) * BLK] for b in range(N_DEV)]
    before = dot(jnp.concatenate(parts, axis=0).astype(BF16), upper)
    run = jnp.zeros((LOC, 1), F32)
    ranks = []
    for b in range(N_DEV):
        ranks.append(before[b * LOC:(b + 1) * LOC, :] + run)
        run = run + jnp.sum(parts[b], axis=1, keepdims=True)
    rank = jnp.concatenate(ranks, axis=1)
    erow = lax.broadcasted_iota(I32, (LOC, 1), 0)
    off_v = jnp.zeros((LOC, 1), F32)
    off = jnp.int32(0)
    for e in range(LOC):
        cnt = jnp.sum(jnp.where(erow == e, run, 0.0)).astype(I32)
        cnt_ref[e] = cnt
        off_s[e] = off
        off_v = jnp.where(erow == e, off.astype(F32), off_v)
        off = off + ((cnt + 15) // 16) * 16
    n_comb = jnp.maximum((off + COMB - 1) // COMB, 1)
    place = rank + off_v
    for j in range(TOP_K):
        mine = jnp.full((1, TOK), -1.0, F32)
        for e in range(LOC):
            mine = jnp.where(local[j] == float(e), place[e:e + 1, :], mine)
        pos[j:j + 1, :] = mine
    ids = jnp.concatenate(local, axis=0)
    gap = jnp.zeros((TOP_K, TOK), F32)
    slots = jnp.concatenate([*three_parts(gate), gap, ids, ids, ids, gap, pos[0:TOP_K, :], jnp.zeros((BLK - 36, TOK), F32)], axis=0)
    for b in range(N_DEV):
        turned = slots[:, b * BLK:(b + 1) * BLK].T
        pos_t[b * BLK:(b + 1) * BLK, :] = turned
        mt[b * BLK:(b + 1) * BLK, :] = turned.astype(BF16)

    sy[...] = jnp.zeros_like(sy)
    sdx[...] = jnp.zeros_like(sdx)
    dacc[...] = jnp.zeros_like(dacc)
    for c in tokens_in:
        c.wait()

    def gather(i, carry):
        r0 = pl.multiple_of(i * GATHER, GATHER)
        rid = (r0 + lax.broadcasted_iota(I32, (GATHER, 1), 0)).astype(F32)
        here = pl.ds(r0, GATHER)
        picks = []
        for kb in range(TOK // 256):
            lanes = slice(kb * 256, (kb + 1) * 256)
            hit = None
            for j in range(TOP_K):
                m = pos[j:j + 1, lanes] == rid
                hit = m if hit is None else hit | m
            picks.append(jnp.where(hit, 1.0, 0.0).astype(BF16))
        pick = jnp.concatenate(picks, axis=1)
        xs[here, :] = dot(pick, xgy[0]).astype(BF16)
        gys[here, :] = dot(pick, xgy[1]).astype(BF16)
        mrow[here, :] = dot(pick, mt[...]).astype(BF16)
        os_[here, :] = jnp.zeros((GATHER, DIM), BF16)
        ps[here, :] = jnp.zeros((GATHER, DIM + BLK), BF16)
        gcol[here, :] = jnp.zeros((GATHER, 1), F32)
        return carry

    lax.fori_loop(0, n_comb, gather, 0)

    def chunks(size, items, left=None, between=iter(())):
        lane = lax.broadcasted_iota(I32, (size, BLK), 1)
        heres = [pl.ds(pl.multiple_of(it[1], 16), size) for it in items]
        xv = [xs[h, :] for h in heres]
        credit = [0.0]

        def tiled(width, cost, product):
            tiles = []
            for n in range(0, width, 256):
                m = min(n + 256, width)
                tiles.append(product(n, m))
                credit[0] += cost * (m - n) / 256
                while credit[0] >= 1.0:
                    next(between, None)
                    credit[0] -= 1.0
            return jnp.concatenate(tiles, axis=1)

        uv = [tiled(2 * DIM, 0.36, lambda n, m, x=x, it=it: dot(x, wgu[it[3], :, n:m])) for x, it in zip(xv, items)]
        gy = [gys[h, :].astype(F32) for h in heres]
        ms = [mrow[h, :].astype(F32) for h in heres]
        match = [(lane < 3 * TOP_K) & (pltpu.roll(m, BLK - 16, 1) == it[0].astype(F32)) for m, it in zip(ms, items)]
        g = [jnp.sum(jnp.where(k, m, 0.0), axis=1, keepdims=True) for k, m in zip(match, ms)]
        q = [(a * b).astype(BF16) for a, b in zip(g, gy)]
        r = [tiled(DIM, 0.85, lambda n, m, a=a, it=it: dot(a, wd[it[2], n:m, :], ((1,), (1,)))) for a, it in zip(q, items)]
        u = [a[:, :DIM].astype(BF16).astype(F32) for a in uv]
        v = [a[:, DIM:].astype(BF16).astype(F32) for a in uv]
        s = [jax.nn.sigmoid(a) for a in u]
        act = [(a * b * c).astype(BF16) for a, b, c in zip(u, s, v)]
        o = [tiled(DIM, 0.43, lambda n, m, a=a, it=it: dot(a, wd[it[2], :, n:m])).astype(BF16) for a, it in zip(act, items)]
        dv = [(a * b * c).astype(BF16) for a, b, c in zip(r, u, s)]
        du = [(a * b * c * (1.0 + d * (1.0 - c))).astype(BF16) for a, b, c, d in zip(r, v, s, u)]
        duv = [jnp.concatenate([a, b], axis=1) for a, b in zip(du, dv)]
        for i, h in enumerate(heres):
            dgate = jnp.sum(gy[i] * o[i].astype(F32), axis=1, keepdims=True)
            hi, mid, low = three_parts(dgate)
            spread = jnp.where(lane < TOP_K, hi, jnp.where(lane < 2 * TOP_K, mid, low))
            dgs = jnp.where(match[i], spread, 0.0).astype(BF16)
            if left is None:
                os_[h, :] = o[i]
                ps[h, DIM:] = dgs
                gcol[h, :] = g[i]
            else:
                p = dot(duv[i], wgu[items[i][3]], ((1,), (1,))).astype(BF16)
                pd = jnp.concatenate([p, dgs], axis=1)
                keep = lax.broadcasted_iota(I32, (size, 1), 0) < left
                os_[h, :] = jnp.where(keep, o[i].astype(F32), os_[h, :].astype(F32)).astype(BF16)
                ps[h, :] = jnp.where(keep, pd.astype(F32), ps[h, :].astype(F32)).astype(BF16)
                gcol[h, :] = jnp.where(keep, g[i], gcol[h, :])
            stage = items[i][4]
            stage[:, 0:DIM] = xv[i]
            stage[:, DIM:2 * DIM] = act[i]
            stage[:, 2 * DIM:3 * DIM] = q[i]
            stage[:, 3 * DIM:5 * DIM] = duv[i]

    def input_grads(items):
        for _, base, _, wide, stage in items:
            duv = stage[:, 3 * DIM:5 * DIM]
            for d in range(0, DIM, 128):
                p = dot(wgu[wide, d:d + 128, :], duv, ((1,), (1,))).T.astype(BF16)
                ps[pl.ds(pl.multiple_of(base, 16), SMALL), d:d + 128] = p
                yield

    def small(e):
        return (e, off_s[e], lax.rem(e, RING), lax.rem(e, RING + 2), stage_s.at[lax.rem(e, 4)])

    def earlier(e, i):
        before = lax.rem(e + LOC - 2, LOC)
        return (before, jnp.where(i > 0, off_s[before], ROWS - SMALL), 0, lax.rem(e + RING, RING + 2), stage_s.at[lax.rem(e + 2, 4)])

    def small_out(e):
        buf = lax.rem(e, 4)
        return pltpu.make_async_copy(stage_s.at[buf], rows_hbm.at[e, pl.ds(0, SMALL)], s_sem.at[buf])

    def big_out(e, b):
        return pltpu.make_async_copy(stage_b, rows_hbm.at[e, pl.ds(pl.multiple_of(SMALL + b * BIG, 32), BIG)], b_sem)

    def pair(i, sent):
        both = [2 * i, 2 * i + 1]
        for e in both:
            for c in weights(e):
                c.wait()

        @pl.when(i >= 2)
        def _():
            for e in both:
                small_out(e - 4).wait()

        between = input_grads([earlier(e, i) for e in both])
        chunks(SMALL, [small(e) for e in both], between=between)
        for _ in between:
            pass
        for e in both:
            small_out(e).start()
        for e in both:
            def big(b, n, e=e):
                @pl.when(n > 0)
                def _():
                    big_out(e, b).wait()

                base = SMALL + b * BIG
                chunks(BIG, [(e, off_s[e] + base, lax.rem(e, RING), lax.rem(e, RING + 2), stage_b)], cnt_ref[e] - base)
                big_out(e, b).start()
                return n + 1

            sent = lax.fori_loop(0, (jnp.maximum(cnt_ref[e] - SMALL, 0) + BIG - 1) // BIG, big, sent)

        @pl.when(i + 2 < LOC // 2)
        def _():
            for e in both:
                for c in weights(e + RING):
                    c.start()

        return sent

    sent = lax.fori_loop(0, LOC // 2, pair, jnp.int32(0))
    for _ in input_grads([small(jnp.int32(e)) for e in (LOC - 2, LOC - 1)]):
        pass
    for e in range(4):
        small_out(jnp.int32(e)).wait()

    @pl.when(sent > 0)
    def _():
        big_out(jnp.int32(0), 0).wait()

    def leave(n):
        r, c, k = n // 4, (n // 2) % 2, n % 2
        dr, dc, dk = lax.rem(row + r, 2), lax.rem(col + c, 2), lax.rem(core + k, 2)
        for far in range(2):
            for send in range(2):
                @pl.when((dk == send) & (dc == far))
                def _():
                    pltpu.make_async_copy(sy.at[n], sums[far][send].at[dr], out_sem.at[n, 0]).start()

                @pl.when((dk == send) & (dr == far))
                def _():
                    pltpu.make_async_copy(sdx.at[n], sums[far][send].at[2 + dc, pl.ds(0, BLK)], out_sem.at[n, 1]).start()

    def combine(i, last):
        r0 = pl.multiple_of(i * COMB, COMB)
        here = pl.ds(r0, COMB)
        hi, mid, low = three_parts(gcol[here, :] * os_[here, :].astype(F32))
        tri[0:COMB, :] = hi.astype(BF16)
        tri[COMB:2 * COMB, :] = mid.astype(BF16)
        tri[2 * COMB:, :] = low.astype(BF16)
        rid = (r0 + lax.broadcasted_iota(I32, (1, COMB), 1)).astype(F32)
        for t in range(TOK // 256):
            toks = slice(t * 256, (t + 1) * 256)
            hit = None
            for j in range(TOP_K):
                m = pos_t[toks, 32 + j:33 + j] == rid
                hit = m if hit is None else hit | m
            pick = jnp.where(hit, 1.0, 0.0).astype(BF16)
            yb = dot(jnp.concatenate([pick] * 3, axis=1), tri[...])
            db = dot(pick, ps[here, :])
            for k in range(2):
                n = 2 * t + k
                half = slice(k * BLK, (k + 1) * BLK)
                sy[n, 0:BLK, :] += yb[half]
                sdx[n, :, :] += db[half, :DIM]
                dacc[n, :, :] += db[half, DIM:]
                if last:
                    dgt = dacc[n, :, :].T
                    sy[n, BLK:BLK + TOP_K, 0:BLK] = (dgt[0:TOP_K] + dgt[TOP_K:2 * TOP_K]) + dgt[2 * TOP_K:3 * TOP_K]
                    leave(n)

    def combine_step(i, carry):
        combine(i, False)
        return carry

    lax.fori_loop(0, n_comb - 1, combine_step, 0)
    combine(n_comb - 1, True)
    for n in range(N_DEV):
        pltpu.make_async_copy(sy.at[n], near_k.at[0], out_sem.at[n, 0]).wait()
        pltpu.make_async_copy(sdx.at[n], near_k.at[2, pl.ds(0, BLK)], out_sem.at[n, 1]).wait()


def run_experts(meta_all, xg, w_gate, w_up, w_down):
    vmem = pl.BlockSpec(memory_space=pltpu.VMEM)
    hbm = pl.BlockSpec(memory_space=pl.ANY)
    sums = jax.ShapeDtypeStruct((4, BLK + 8, DIM), F32)
    return pl.pallas_call(
        expert_kernel,
        out_shape=(*[sums] * 4, jax.ShapeDtypeStruct((LOC, SLAB, 5 * DIM), BF16), jax.ShapeDtypeStruct((LOC,), I32)),
        in_specs=[vmem, hbm, hbm, hbm, hbm],
        out_specs=(*[hbm] * 5, pl.BlockSpec(memory_space=pltpu.SMEM)),
        scratch_shapes=[
            pltpu.VMEM((2, TOK, DIM), BF16), pltpu.VMEM((TOK, BLK), BF16),
            pltpu.VMEM((RING + 2, DIM, 2 * DIM), BF16), pltpu.VMEM((RING, DIM, DIM), BF16),
            pltpu.VMEM((ROWS, DIM), BF16), pltpu.VMEM((ROWS, DIM), BF16), pltpu.VMEM((ROWS, BLK), BF16),
            pltpu.VMEM((ROWS, DIM), BF16), pltpu.VMEM((ROWS, DIM + BLK), BF16), pltpu.VMEM((ROWS, 1), F32),
            pltpu.VMEM((8, TOK), F32), pltpu.VMEM((TOK, BLK), F32), pltpu.VMEM((3 * COMB, DIM), BF16),
            pltpu.VMEM((N_DEV, BLK + 8, DIM), F32), pltpu.VMEM((N_DEV, BLK, DIM), F32), pltpu.VMEM((N_DEV, BLK, BLK), F32),
            pltpu.SMEM((LOC,), I32),
            pltpu.VMEM((4, SMALL, 5 * DIM), BF16), pltpu.VMEM((BIG, 5 * DIM), BF16),
            pltpu.SemaphoreType.DMA((2,)), pltpu.SemaphoreType.DMA((RING, 3)), pltpu.SemaphoreType.DMA((4,)), pltpu.SemaphoreType.DMA,
            pltpu.SemaphoreType.DMA((N_DEV, 2)),
        ],
        compiler_params=pltpu.CompilerParams(vmem_limit_bytes=VMEM_MAX),
        cost_estimate=pl.CostEstimate(flops=6_000_000_000, bytes_accessed=60_000_000, transcendentals=0),
        name="expert_rows",
    )(meta_all, xg, w_gate, w_up, w_down)


def wgrad_kernel(lo, hi, n_alias, cnt_ref, rows_hbm, *refs):
    gg_hbm, gu_hbm, gd_hbm = refs[n_alias:n_alias + 3]
    small, big, out_gu, out_d, r_sem, b_sem, o_sem = refs[n_alias + 3:]

    def rows_in(i):
        return pltpu.make_async_copy(rows_hbm.at[lo + i, pl.ds(0, SMALL)], small.at[lax.rem(i, 2)], r_sem.at[lax.rem(i, 2)])

    def piece_in(i, b):
        return pltpu.make_async_copy(rows_hbm.at[lo + i, pl.ds(pl.multiple_of(b * PIECE, PIECE), PIECE)], big.at[lax.rem(i, 2)], b_sem.at[lax.rem(i, 2)])

    def fetch(i):
        many = cnt_ref[lo + i] > SMALL

        @pl.when(many)
        def _():
            piece_in(i, 0).start()

        @pl.when(jnp.logical_not(many))
        def _():
            rows_in(i).start()

    def results(i):
        slot, e = lax.rem(i, 2), lo + i
        return (pltpu.make_async_copy(out_gu.at[slot, :, pl.ds(0, DIM)], gg_hbm.at[e], o_sem.at[slot, 0]),
                pltpu.make_async_copy(out_gu.at[slot, :, pl.ds(DIM, DIM)], gu_hbm.at[e], o_sem.at[slot, 1]),
                pltpu.make_async_copy(out_d.at[slot], gd_hbm.at[e], o_sem.at[slot, 2]))

    def products(ref, size, left):
        keep = lax.broadcasted_iota(I32, (size, 1), 0) < left
        part = lambda a, b: jnp.where(keep, ref[:, a * DIM:b * DIM].astype(F32), 0.0).astype(BF16)
        x, a, q, duv = part(0, 1), part(1, 2), part(2, 3), part(3, 5)
        return dot(x, duv, ((0,), (0,))), dot(a, q, ((0,), (0,)))

    fetch(jnp.int32(0))

    def expert(i, carry):
        slot = lax.rem(i, 2)
        cnt = cnt_ref[lo + i]

        @pl.when(i + 1 < hi - lo)
        def _():
            fetch(i + 1)

        @pl.when(i >= 2)
        def _():
            for c in results(i - 2):
                c.wait()

        @pl.when(cnt <= SMALL)
        def _():
            rows_in(i).wait()
            g1, g2 = products(small.at[slot], SMALL, cnt)
            out_gu[slot] = g1
            out_d[slot] = g2

        @pl.when(cnt > SMALL)
        def _():
            piece_in(i, 0).wait()
            g1, g2 = products(big.at[slot], PIECE, cnt)
            out_gu[slot] = g1
            out_d[slot] = g2

            def more(b, c2):
                piece_in(i, b).start()
                piece_in(i, b).wait()
                g1, g2 = products(big.at[slot], PIECE, cnt - b * PIECE)
                out_gu[slot] += g1
                out_d[slot] += g2
                return c2

            lax.fori_loop(1, (cnt + PIECE - 1) // PIECE, more, 0)

        for c in results(i):
            c.start()
        return carry

    lax.fori_loop(0, hi - lo, expert, 0)
    for i in (hi - lo - 2, hi - lo - 1):
        for c in results(jnp.int32(i)):
            c.wait()


def weight_grads(lo, hi, cnt, rows, earlier=()):
    hbm = pl.BlockSpec(memory_space=pl.ANY)
    out = jax.ShapeDtypeStruct((LOC, DIM, DIM), F32)
    return pl.pallas_call(
        functools.partial(wgrad_kernel, lo, hi, len(earlier)),
        out_shape=(out, out, out),
        in_specs=[pl.BlockSpec(memory_space=pltpu.SMEM), hbm] + [hbm] * len(earlier),
        out_specs=(hbm, hbm, hbm),
        input_output_aliases={2 + i: i for i in range(len(earlier))},
        scratch_shapes=[
            pltpu.VMEM((2, SMALL, 5 * DIM), BF16), pltpu.VMEM((2, PIECE, 5 * DIM), BF16),
            pltpu.VMEM((2, DIM, 2 * DIM), F32), pltpu.VMEM((2, DIM, DIM), F32),
            pltpu.SemaphoreType.DMA((2,)), pltpu.SemaphoreType.DMA((2,)), pltpu.SemaphoreType.DMA((2, 3)),
        ],
        compiler_params=pltpu.CompilerParams(vmem_limit_bytes=36 * 1024 * 1024),
        cost_estimate=pl.CostEstimate(flops=(hi - lo) * 400_000_000, bytes_accessed=(hi - lo) * 5_000_000, transcendentals=0),
        name="weight_grads",
    )(cnt, rows, *earlier)


def solution(mesh):
    tok_spec = P(None, ALL_AXES, None)
    w_spec = P(ALL_AXES, None, None)

    def swap(value, axis):
        return lax.ppermute(value, axis, [(0, 1), (1, 0)])

    def moe_layer(x, route_idx, gates, w_gate, w_up, w_down, grad_y):
        tok_dev = x.shape[1]
        flat = lambda a: a.reshape(2 * tok_dev, -1)
        turn = lambda a: jnp.transpose(a, (0, 2, 1))
        xg, meta_all = all_gather_tokens(flat(x), flat(grad_y), turn(route_idx), turn(gates))
        near_k, near_s, far_k, far_s, rows, cnt = run_experts(meta_all, xg.reshape(2, TOK, DIM), w_gate, w_up, w_down)
        far_in = swap(far_s, "core")
        y_in = swap(far_k[:2] + far_in[:2], "col")
        dx_in = swap(far_k[2:, :BLK] + far_in[2:, :BLK], "row")
        near_in = swap(near_s, "core")
        early = weight_grads(0, 9, cnt, rows)
        y_out = near_k[1] + near_in[1] + y_in[1]
        dx_out = near_k[3, :BLK] + near_in[3, :BLK] + dx_in[1]
        y_out, dx_out, early = lax.optimization_barrier((y_out, dx_out, early))
        y_far, dx_far = swap(y_out, "row"), swap(dx_out, "col")
        g_gate, g_up, g_down = weight_grads(9, LOC, cnt, rows, early)
        y = (near_k[0, :BLK] + near_in[0, :BLK] + y_in[0, :BLK] + y_far[:BLK]).astype(BF16).reshape(x.shape)
        dx = (near_k[2, :BLK] + near_in[2, :BLK] + dx_in[0] + dx_far).astype(BF16).reshape(x.shape)
        tail = slice(BLK, BLK + TOP_K)
        dg = near_k[0, tail, :BLK] + near_in[0, tail, :BLK] + y_in[0, tail, :BLK] + y_far[tail, :BLK]
        dg = turn(jnp.stack([dg[:, m * tok_dev:(m + 1) * tok_dev] for m in range(2)]))
        return y, dx, dg, g_gate, g_up, g_down

    return jax.shard_map(moe_layer, mesh=mesh, in_specs=(tok_spec, tok_spec, tok_spec, w_spec, w_spec, w_spec, tok_spec), out_specs=(tok_spec, tok_spec, tok_spec, w_spec, w_spec, w_spec), check_vma=False)
```
